128 devices in a mesh: gx: 16 (over y_hi, z, core), gy: 8 (over y_lo, x).
Axes of the slice: x: 4, y: 4 (y_hi: 2, y_lo: 2; y = y_hi * 2 + y_lo), z: 4, core: 2. Of those that a mesh axis runs over, the one named last changes fastest.
Arguments:
- proof: bfloat16 [2048, 256, 512], P(('gx', 'gy')), may hold values from -24 to 24
- target: bfloat16 [64, 256, 512], P('gx', 'gy'), may hold values from -6 to 6
- loading: float32 [256], replicated, may hold values from 2 to 32
Outputs:
- predicted: float32 [64, 256, 512], P('gx', 'gy')
The draws below stay inside these ranges and needn't reach their ends.
All inputs are finite; a program needn't handle non-finite values.
Results may differ from the reference program's by a relative error of at most 0.0049.
The reference program's roundings to bfloat16 on the way count: a program that leaves them out, or rounds other values in their place, can miss the bound.
Values may be sent and summed in bfloat16 or wider, within the bound.
A program may use at most 128 MiB of HBM per device.

```python
import math
import jax
import jax.numpy as jnp
from jax import lax

W = 2048
P_SIZE = 64
L = 512
S = 256
F = 256


def strengthened(drawn, stream_key, source, target, blocks, factor):
    owner, partner = [(jnp.arange(drawn.shape[dim]) // (drawn.shape[dim] // blocks)).reshape([-1 if axis == dim else 1 for axis in range(drawn.ndim)]) for dim in (source, target)]
    chosen = jax.random.permutation(stream_key, blocks)[partner]
    strong = (owner == chosen) | (owner == (partner + blocks // 2) % blocks)
    return jnp.where(strong, factor * drawn, drawn)


def levels(rng, extent, shards, least, largest):
    def one(position, blocks):
        draws = jax.random.uniform(jax.random.fold_in(jax.random.fold_in(rng, 6), position), (blocks,), jnp.float32, least / len(shards), largest / len(shards))
        return jnp.repeat(jnp.exp(draws), extent[position] // blocks).reshape((-1,) + (1,) * (len(extent) - position - 1))

    loudness = one(*shards[0])
    for cut in shards[1:]:
        loudness = loudness * one(*cut)
    return loudness


def bell_draw(key, dims, deviation, bound, cuts=(), kind=jnp.bfloat16):
    drawn = jax.random.normal(key, dims, jnp.float32) * deviation
    if len(cuts) > 0:
        drawn = levels(key, dims, cuts, -0.22, 0.18) * drawn
    return jnp.clip(drawn, min=-bound, max=bound).astype(kind)


def noise_with(key, extent, deviation, bound, split, heavy, kind=jnp.bfloat16):
    entries = deviation * jax.random.normal(key, extent, jnp.float32)
    if split:
        entries = entries * levels(key, extent, split, -0.22, 0.18)
    return jnp.clip(strengthened(entries, jax.random.fold_in(key, 3), *heavy), -bound, bound).astype(kind)


def setup_inputs(seed: int = 0) -> dict:
    key_of = jax.random.split(jax.random.key(seed), 4)
    return {
        "proof": noise_with(key_of[0], (W, S, L), 1.0, 24.0, ((0, 128),), (0, 1, 128, 5.5)),
        "target": bell_draw(key_of[1], (P_SIZE, S, L), 1.0, 6.0, ((0, 16), (1, 8))),
        "loading": jnp.clip(jnp.exp(jax.random.uniform(key_of[2], (F,), jnp.float32, math.log(2.0), math.log(32.0))), 2.0, 32.0),
    }


def transform_tables(length):
    half = length // 2
    sample = jnp.arange(length, dtype=jnp.int32)
    freq_bin = jnp.arange(half, dtype=jnp.int32)
    phase = (freq_bin[:, None] * sample[None, :] % length).astype(jnp.float32) * (2.0 * math.pi / length)
    window = 0.5 - 0.5 * jnp.cos(sample.astype(jnp.float32) * (2.0 * math.pi / length))
    forward = jnp.stack([window * jnp.cos(phase), -window * jnp.sin(phase)], axis=1).reshape(length, length)
    forward = forward * (1.0 / math.sqrt(0.375 * length))
    inverse = jnp.stack([jnp.cos(phase), -jnp.sin(phase)], axis=1).reshape(length, length) * math.sqrt(2.0 / length)
    return (forward.astype(jnp.bfloat16), inverse.astype(jnp.bfloat16))

def contract(left, right):
    return lax.dot_general(left, right, (((1,), (1,)), ((), ())), preferred_element_type=jnp.float32)

def project(left, right):
    return lax.dot_general(left, right, (((0,), (0,)), ((), ())), preferred_element_type=jnp.float32)

def reference(proof, target, loading):
    length = proof.shape[2]
    channels = proof.shape[0]
    targets = target.shape[0]
    segments = proof.shape[1]
    forward, inverse = transform_tables(length)
    wit_spec = lax.dot_general(forward, proof, (((1,), (2,)), ((), ())), preferred_element_type=jnp.float32).astype(jnp.bfloat16)
    tar_spec = lax.dot_general(forward, target, (((1,), (2,)), ((), ())), preferred_element_type=jnp.float32).astype(jnp.bfloat16)
    wit_bins = wit_spec.reshape(length // 2, 2, channels, segments)
    tar_bins = tar_spec.reshape(length // 2, 2, targets, segments)
    rho = (1.0 + math.sqrt(channels / segments)) ** 2

    def per_bin(items):
        wit, tar, load_val = items
        wit_re, wit_im = (wit[0], wit[1])
        tar_re, tar_im = (tar[0], tar[1])
        gram_re = ((contract(wit_re, wit_re) + contract(wit_im, wit_im)) / segments).astype(jnp.bfloat16)
        gram_im = ((contract(wit_im, wit_re) - contract(wit_re, wit_im)) / segments).astype(jnp.bfloat16)
        rhs_re = (contract(wit_re, tar_re) + contract(wit_im, tar_im)) / segments
        rhs_im = (contract(wit_im, tar_re) - contract(wit_re, tar_im)) / segments
        step_size = 1.0 / (load_val + rho)
        first_re = step_size * rhs_re
        first_im = step_size * rhs_im
        half_re = first_re.astype(jnp.bfloat16)
        half_im = first_im.astype(jnp.bfloat16)
        image_re = jnp.dot(gram_re, half_re, preferred_element_type=jnp.float32) - jnp.dot(gram_im, half_im, preferred_element_type=jnp.float32)
        image_im = jnp.dot(gram_re, half_im, preferred_element_type=jnp.float32) + jnp.dot(gram_im, half_re, preferred_element_type=jnp.float32)
        second_re = (first_re + step_size * (rhs_re - image_re - load_val * first_re)).astype(jnp.bfloat16)
        second_im = (first_im + step_size * (rhs_im - image_im - load_val * first_im)).astype(jnp.bfloat16)
        pred_re = project(second_re, wit_re) + project(second_im, wit_im)
        pred_im = project(second_re, wit_im) - project(second_im, wit_re)
        return jnp.stack([pred_re, pred_im]).astype(jnp.bfloat16)
    preds = lax.map(per_bin, (wit_bins, tar_bins, loading))
    preds = preds.reshape(length, targets, segments)
    return lax.dot_general(preds, inverse, (((0,), (0,)), ((), ())), preferred_element_type=jnp.float32)
```

```python
import functools
import math

import jax
import jax.numpy as jnp
import numpy as np
from jax import lax
from jax.experimental import pallas as pl
from jax.experimental.pallas import tpu as pltpu
from jax.sharding import PartitionSpec as P

GROUPS = 8
POSITIONS = 16
PHASES = 4
CHANNELS = 16
STRIDE = 264
MESH = pl.DeviceIdType.MESH


def transform_tables(length):
    half = length // 2
    sample = np.arange(length)
    phase = ((np.arange(half)[:, None] * sample[None, :]) % length).astype(np.float32) * np.float32(
        2.0 * math.pi / length
    )
    angle = sample.astype(np.float32) * np.float32(2.0 * math.pi / length)
    window = np.float32(0.5) - np.float32(0.5) * np.cos(angle)
    forward = np.stack([window * np.cos(phase), -window * np.sin(phase)], axis=1).reshape(
        length, length
    ) * np.float32(1.0 / math.sqrt(0.375 * length))
    inverse = np.stack([np.cos(phase), -np.sin(phase)], axis=1).reshape(
        length, length
    ) * np.float32(math.sqrt(2.0 / length))
    return forward.astype(np.float32), inverse.astype(np.float32)


def split_place(gx, gy):
    core, z, yh = gx % 2, (gx // 2) % 4, gx // 8
    x, yl = gy % 4, gy // 4
    vx, vz, vy = x // 2, z // 2, yh
    ux, uz, uy = (x + vx) % 2, (z + vz) % 2, (yl + yh) % 2
    return vz * 4 + vy * 2 + vx, uz * 4 + uy * 2 + ux, core


def join_place(v, u, core):
    vx, vy, vz = v % 2, (v // 2) % 2, v // 4
    ux, uy, uz = u % 2, (u // 2) % 2, u // 4
    x = 2 * vx + (ux + vx) % 2
    z = 2 * vz + (uz + vz) % 2
    return vy * 8 + z * 2 + core, ((uy + vy) % 2) * 4 + x


def bins_of(v, u, core):
    return (u * 2 + core) * GROUPS + v, 128 + (v * 2 + core) * GROUPS + u


def nt(left, right):
    return lax.dot_general(
        left, right, (((1,), (1,)), ((), ())), preferred_element_type=jnp.float32
    )


def nn(left, right):
    return lax.dot_general(
        left, right, (((1,), (0,)), ((), ())), preferred_element_type=jnp.float32
    )


def tn(left, right):
    return lax.dot_general(
        left, right, (((0,), (0,)), ((), ())), preferred_element_type=jnp.float32
    )


def kernel(
    rho,
    tab_hbm, ttab_hbm, inv_hbm, proof_hbm, target_hbm, loading,
    out,
    tab, ttab, inv, proof, target,
    stage, xsend, xrecv, msend, mrecv, macc, tmat, tsend, trecv, rows, psend, precv,
    proof_sem, tab_sem, small_sem,
    x_send_sem, x_recv_sem, m_send_sem, m_recv_sem, t_sem, p_sem,
):
    gx, gy = lax.axis_index("gx"), lax.axis_index("gy")
    v, u, core = split_place(gx, gy)
    me = gx * 8 + gy
    group = (v, u)
    position = (u * 2 + core, v * 2 + core)

    def place_of(cls, pos):
        if cls == 0:
            return join_place(v, pos // 2, pos % 2)
        return join_place(pos // 2, u, pos % 2)

    def home_of(cls, grp):
        return join_place(grp, u, core) if cls == 0 else join_place(v, grp, core)

    def pair_of(cls, phase):
        return (group[cls] // 2 + 1 + phase) % 4

    tab_copies = []
    for block in range(2 * PHASES):
        phase, cls = block // 2, block % 2
        tab_copies.append(
            pltpu.make_async_copy(
                tab_hbm.at[cls * 4 + pair_of(cls, phase)], tab.at[block], tab_sem.at[block]
            )
        )
    for copy in tab_copies[:4]:
        copy.start()

    def proof_copy(c):
        return pltpu.make_async_copy(proof_hbm.at[c], proof.at[c], proof_sem.at[c])

    for c in range(CHANNELS):
        proof_copy(c).start()
    for copy in tab_copies[4:]:
        copy.start()
    small = [
        pltpu.make_async_copy(target_hbm, target, small_sem.at[0]),
        pltpu.make_async_copy(ttab_hbm, ttab, small_sem.at[1]),
        pltpu.make_async_copy(inv_hbm, inv, small_sem.at[2]),
    ]
    for copy in small:
        copy.start()

    barrier = pltpu.get_barrier_semaphore()

    def greet(d, carry):
        other = (me + d) % 128
        pl.semaphore_signal(
            barrier, inc=1, device_id=(other // 8, other % 8), device_id_type=MESH
        )
        return carry

    lax.fori_loop(1, 128, greet, 0)

    def spectra(half, first):
        base = half * 4

        def channel(c, carry):
            if first:
                proof_copy(c).wait()
            got = nt(tab[base : base + 4].reshape(256, 512), proof[c])
            start = pl.multiple_of(c * STRIDE, 8)
            stage[0, pl.ds(start, 256), :] = got[:, :128]
            stage[1, pl.ds(start, 256), :] = got[:, 128:]
            return carry

        lax.fori_loop(0, CHANNELS, channel, 0)

    def turn(block):
        base = (block % 4) * 64

        def one(r, carry):
            low = stage[0, pl.ds(base + r, CHANNELS, stride=STRIDE), :]
            high = stage[1, pl.ds(base + r, CHANNELS, stride=STRIDE), :]
            xsend[block * 64 + r, :, 0:128] = low.astype(jnp.bfloat16)
            xsend[block * 64 + r, :, 128:256] = high.astype(jnp.bfloat16)
            return carry

        lax.fori_loop(0, 64, one, 0, unroll=8)

    def send_block(block):
        cls = block % 2
        mine = position[cls]

        def one(d, carry):
            pos = (mine + d) % POSITIONS
            pltpu.make_async_remote_copy(
                src_ref=xsend.at[pl.ds(block * 64 + pos * 4, 4)],
                dst_ref=xrecv.at[block, :, mine],
                send_sem=x_send_sem.at[block],
                recv_sem=x_recv_sem.at[block],
                device_id=place_of(cls, pos),
                device_id_type=MESH,
            ).start()
            return carry

        lax.fori_loop(1, POSITIONS, one, 0)
        for i in range(4):
            xrecv[block, i, mine] = xsend[block * 64 + mine * 4 + i]

    for copy in tab_copies[:4]:
        copy.wait()
    spectra(0, True)
    turn(0)
    turn(1)
    pl.semaphore_wait(barrier, 127)
    send_block(0)
    send_block(1)
    turn(2)
    turn(3)
    send_block(2)
    send_block(3)
    for copy in tab_copies[4:]:
        copy.wait()
    spectra(1, False)
    for block in range(4, 8):
        turn(block)
        send_block(block)

    for copy in small:
        copy.wait()
    rows[...] = nt(ttab[...], target[...])

    def pack_rows(dst):
        def one(d, carry):
            dst[d] = rows[pl.ds(d * 4, 4), :].astype(jnp.bfloat16)
            return carry

        lax.fori_loop(0, 128, one, 0, unroll=8)

    def unpack_rows(src):
        def one(d, carry):
            rows[pl.ds(d * 4, 4), :] = src[d].astype(jnp.float32)
            return carry

        lax.fori_loop(0, 128, one, 0, unroll=8)

    def send_small(src, dst, sems):
        def one(d, carry):
            other = (me + d) % 128
            pltpu.make_async_remote_copy(
                src_ref=src.at[other],
                dst_ref=dst.at[me],
                send_sem=sems.at[0],
                recv_sem=sems.at[1],
                device_id=(other // 8, other % 8),
                device_id_type=MESH,
            ).start()
            return carry

        lax.fori_loop(1, 128, one, 0)
        dst[me] = src[me]

    def wait_bytes(view, sem):
        pltpu.make_async_copy(view, view, sem).wait()

    pack_rows(tsend)
    send_small(tsend, trecv, t_sem)

    def partial_gram(block, which):
        re = xrecv[block, which * 2].reshape(256, 256)
        im = xrecv[block, which * 2 + 1].reshape(256, 256)
        ret, imt = re.T, im.T
        return (nn(ret, re) + nn(imt, im) + (nn(ret, im) - nn(imt, re))) * (1.0 / 256.0)

    def gram_copy(block, slot, grp, cls):
        return pltpu.make_async_remote_copy(
            src_ref=msend.at[block, slot],
            dst_ref=mrecv.at[cls, group[cls]],
            send_sem=m_send_sem.at[cls],
            recv_sem=m_recv_sem.at[cls],
            device_id=home_of(cls, grp),
            device_id_type=MESH,
        )

    for block in range(8):
        phase, cls = block // 2, block % 2
        wait_bytes(xrecv.at[block, :, pl.ds(0, POSITIONS - 1)], x_recv_sem.at[block])
        if phase < PHASES - 1:
            for which in range(2):
                msend[block, which] = partial_gram(block, which).astype(jnp.bfloat16)
                gram_copy(block, which, pair_of(cls, phase) * 2 + which, cls).start()
        else:
            other = (group[cls] + 1) % 2
            msend[block, 0] = partial_gram(block, other).astype(jnp.bfloat16)
            gram_copy(block, 0, pair_of(cls, phase) * 2 + other, cls).start()
    for cls in range(2):
        macc[cls] = partial_gram(6 + cls, group[cls] % 2)

    lane = lax.broadcasted_iota(jnp.int32, (16, 128), 1) // 32
    wait_bytes(trecv.at[pl.ds(0, 127)], t_sem.at[1])
    unpack_rows(trecv)
    for i in range(4):
        blocks = [rows[pl.ds(g * 4 + i, 16, stride=32), :] for g in range(8)]
        for t in range(4):
            for tile in range(2):
                total = jnp.zeros((16, 128), jnp.float32)
                for k in range(4):
                    turned = blocks[tile * 4 + k]
                    if k != t:
                        turned = pltpu.roll(turned, (32 * (k - t)) % 128, 1)
                    total = jnp.where(lane == k, turned, total)
                tmat[
                    i // 2, (i % 2) * 64 + t * 16 : (i % 2) * 64 + t * 16 + 16,
                    tile * 128 : tile * 128 + 128,
                ] = total.astype(jnp.bfloat16)

    bins = bins_of(v, u, core)
    for cls in range(2):
        wait_bytes(mrecv.at[cls, pl.ds(0, GROUPS - 1)], m_recv_sem.at[cls])
        gram = macc[cls]
        for n in range(1, GROUPS):
            gram = gram + mrecv[cls, (group[cls] + n) % GROUPS].astype(jnp.float32)
        high = gram.astype(jnp.bfloat16)
        low = (gram - high.astype(jnp.float32)).astype(jnp.bfloat16)

        def combine(straight, turned):
            return (
                0.5 * (straight[:64] - straight[64:] + turned[:64] + turned[64:]),
                0.5 * (straight[:64] + straight[64:] - turned[:64] + turned[64:]),
            )

        left = tmat[cls]
        once_re, once_im = combine(
            nn(left, high) + nn(left, low), nt(left, high) + nt(left, low)
        )
        once = jnp.concatenate([once_re, once_im], axis=0)
        once_high = once.astype(jnp.bfloat16)
        once_low = (once - once_high.astype(jnp.float32)).astype(jnp.bfloat16)
        both = jnp.concatenate([once_high, once_low], axis=0)
        straight, turned = nn(both, high), nt(both, high)
        twice_re, twice_im = combine(
            straight[:128] + straight[128:] + nn(once_high, low),
            turned[:128] + turned[128:] + nt(once_high, low),
        )
        load = loading[bins[cls]]
        step = 1.0 / (load + rho)
        keep, take = 2.0 * step - load * step * step, step * step
        pred = (keep * once_re - take * twice_re, keep * once_im - take * twice_im)
        for part in range(2):
            for g in range(8):
                k, tile = g % 4, g // 4
                total = jnp.zeros((16, 128), jnp.float32)
                for t in range(4):
                    turned = pred[part][t * 16 : t * 16 + 16, tile * 128 : tile * 128 + 128]
                    if k != t:
                        turned = pltpu.roll(turned, (32 * (t - k)) % 128, 1)
                    total = jnp.where(lane == t, turned, total)
                rows[pl.ds(g * 4 + cls * 2 + part, 16, stride=32), :] = total

    pack_rows(psend)
    send_small(psend, precv, p_sem)
    wait_bytes(precv.at[pl.ds(0, 127)], p_sem.at[1])
    unpack_rows(precv)
    out[...] = tn(rows[...].astype(jnp.bfloat16), inv[...])

    for block in range(8):
        wait_bytes(xrecv.at[block, :, pl.ds(0, POSITIONS - 1)], x_send_sem.at[block])
    for cls in range(2):
        wait_bytes(mrecv.at[cls, pl.ds(0, GROUPS - 1)], m_send_sem.at[cls])
    wait_bytes(trecv.at[pl.ds(0, 127)], t_sem.at[0])
    wait_bytes(precv.at[pl.ds(0, 127)], p_sem.at[0])


def tables(length):
    forward, inverse = transform_tables(length)
    by_pair = (
        forward.reshape(2, POSITIONS, 4, 4, length)
        .transpose(0, 2, 1, 3, 4)
        .reshape(8, POSITIONS * 4, length)
    )
    order = []
    for device in range(128):
        for number in bins_of(*split_place(device // 8, device % 8)):
            order += [2 * number, 2 * number + 1]
    return tuple(
        jnp.asarray(table).astype(jnp.bfloat16)
        for table in (by_pair, forward[order], inverse[order])
    )


def local(proof, target, loading):
    channels, segments, length = proof.shape
    rho = (1.0 + math.sqrt(2048 / segments)) ** 2
    by_pair, by_owner, inverse = tables(length)
    bf16, f32 = jnp.bfloat16, jnp.float32
    hbm = pl.BlockSpec(memory_space=pl.ANY)
    scratch = [
        pltpu.VMEM((8, 64, 512), bf16),
        pltpu.VMEM((512, 512), bf16),
        pltpu.VMEM((512, 512), bf16),
        pltpu.VMEM((16, 256, 512), bf16),
        pltpu.VMEM((128, 512), bf16),
        pltpu.VMEM((2, CHANNELS * STRIDE, 128), f32),
        pltpu.VMEM((512, CHANNELS, 256), bf16),
        pltpu.VMEM((8, 4, POSITIONS, CHANNELS, 256), bf16),
        pltpu.VMEM((8, 2, 256, 256), bf16),
        pltpu.VMEM((2, GROUPS, 256, 256), bf16),
        pltpu.VMEM((2, 256, 256), f32),
        pltpu.VMEM((2, 128, 256), bf16),
        pltpu.VMEM((128, 4, 128), bf16),
        pltpu.VMEM((128, 4, 128), bf16),
        pltpu.VMEM((512, 128), f32),
        pltpu.VMEM((128, 4, 128), bf16),
        pltpu.VMEM((128, 4, 128), bf16),
        pltpu.SemaphoreType.DMA((CHANNELS,)),
        pltpu.SemaphoreType.DMA((8,)),
        pltpu.SemaphoreType.DMA((3,)),
        pltpu.SemaphoreType.DMA((8,)),
        pltpu.SemaphoreType.DMA((8,)),
        pltpu.SemaphoreType.DMA((2,)),
        pltpu.SemaphoreType.DMA((2,)),
        pltpu.SemaphoreType.DMA((2,)),
        pltpu.SemaphoreType.DMA((2,)),
    ]
    result = pl.pallas_call(
        functools.partial(kernel, rho),
        out_shape=jax.ShapeDtypeStruct((128, length), f32),
        in_specs=[hbm] * 5 + [pl.BlockSpec(memory_space=pltpu.SMEM)],
        out_specs=pl.BlockSpec(memory_space=pltpu.VMEM),
        scratch_shapes=scratch,
        compiler_params=pltpu.CompilerParams(
            collective_id=0, has_side_effects=True, vmem_limit_bytes=56 * 2**20
        ),
    )(by_pair, by_owner, inverse, proof, target.reshape(128, length), loading)
    return result.reshape(4, 32, length)


def solution(mesh):
    return jax.shard_map(
        local,
        mesh=mesh,
        in_specs=(P(("gx", "gy"), None, None), P("gx", "gy", None), P()),
        out_specs=P("gx", "gy", None),
        check_vma=False,
    )
```

```python
import functools
import math

import jax
import jax.numpy as jnp
import numpy as np
from jax import lax
from jax.experimental import pallas as pl
from jax.experimental.pallas import tpu as pltpu
from jax.sharding import PartitionSpec as P

GROUPS = 8
POSITIONS = 16
CHANNELS = 16
STRIDE = 520
OTHERS = (2, 4, 8, 14, 3, 5, 9, 15, 6, 12, 10, 7, 13, 11, 1)
PIECE = 128
ORDERS = ((4, 2, 1), (1, 2, 4))
MESH = pl.DeviceIdType.MESH


def transform_tables(length):
    half = length // 2
    sample = np.arange(length)
    phase = ((np.arange(half)[:, None] * sample[None, :]) % length).astype(np.float32) * np.float32(
        2.0 * math.pi / length
    )
    angle = sample.astype(np.float32) * np.float32(2.0 * math.pi / length)
    window = np.float32(0.5) - np.float32(0.5) * np.cos(angle)
    forward = np.stack([window * np.cos(phase), -window * np.sin(phase)], axis=1).reshape(
        length, length
    ) * np.float32(1.0 / math.sqrt(0.375 * length))
    inverse = np.stack([np.cos(phase), -np.sin(phase)], axis=1).reshape(
        length, length
    ) * np.float32(math.sqrt(2.0 / length))
    return forward.astype(np.float32), inverse.astype(np.float32)


def split_place(gx, gy):
    core, z, yh = gx % 2, (gx // 2) % 4, gx // 8
    x, yl = gy % 4, gy // 4
    v = (z // 2, yh, x // 2)
    return v, ((z + v[0]) % 2, (yl + yh) % 2, (x + v[2]) % 2), core


def number(bits):
    return (bits[0] * 2 + bits[1]) * 2 + bits[2]


def bins_of(v, u, core):
    return (
        (number(u) * 2 + core) * GROUPS + number(v),
        128 + (number(v) * 2 + core) * GROUPS + number(u),
    )


def next_bit(offset, piece):
    return next(bit for bit in ORDERS[piece] if offset & bit)


def feeders(offset, piece):
    return [
        other for other in range(1, GROUPS) if other ^ next_bit(other, piece) == offset
    ]


def nt(left, right):
    return lax.dot_general(
        left, right, (((1,), (1,)), ((), ())), preferred_element_type=jnp.float32
    )


def nn(left, right):
    return lax.dot_general(
        left, right, (((1,), (0,)), ((), ())), preferred_element_type=jnp.float32
    )


def tn(left, right):
    return lax.dot_general(
        left, right, (((0,), (0,)), ((), ())), preferred_element_type=jnp.float32
    )


def kernel(
    rho,
    tab_hbm, ttab_hbm, proof_hbm, target_hbm, loading,
    out,
    tab, ttab, proof, target,
    stage, xsend, xrecv, xlast, part, msend, mrecv, tmat, tsend, tpass, trecv, rows, psend, precv,
    proof_sem, tab_sem, small_sem,
    x_send_sem, x_recv_sem, m_send_sem, m_recv_sem, t_sem, p_sem,
):
    gx, gy = lax.axis_index("gx"), lax.axis_index("gy")
    v, u, core = split_place(gx, gy)
    group = (v, u)
    mine = (number(u) * 2 + core, number(v) * 2 + core)

    z, yh, x, yl = (gx // 2) % 4, gx // 8, gy % 4, gy // 4
    z_flip = (2 * v[0] + 1 - z % 2, 2 * (1 - v[0]) + 1 - z % 2)
    x_flip = (2 * v[2] + 1 - x % 2, 2 * (1 - v[2]) + 1 - x % 2)
    yh_flip = (yh, 1 - yh)

    def place(which, offset, flip_core=0):
        there_z = z_flip[which] if offset & 4 else z
        there_yh = yh_flip[which] if offset & 2 else yh
        there_yl = 1 - yl if offset & 2 else yl
        there_x = x_flip[which] if offset & 1 else x
        there_core = 1 - core if flip_core else core
        return there_yh * 8 + there_z * 2 + there_core, there_yl * 4 + there_x

    def flipped(bit, flip):
        return 1 - bit if flip else bit

    def pos_at(cls, offset):
        bits = (u, v)[cls]
        return (
            number([flipped(b, offset & (8 >> n)) for n, b in enumerate(bits)]) * 2
            + flipped(core, offset & 1)
        )

    def pair_at(cls, offset):
        bits = group[cls]
        return flipped(bits[0], offset & 2) * 2 + flipped(bits[1], offset & 1)

    barrier = pltpu.get_barrier_semaphore()

    def tab_copy(block):
        cls, offset = block % 2, 3 - block // 2
        return pltpu.make_async_copy(
            tab_hbm.at[cls * 4 + pair_at(cls, offset)], tab.at[block], tab_sem.at[block]
        )

    def proof_copy(c):
        return pltpu.make_async_copy(proof_hbm.at[c], proof.at[c], proof_sem.at[c])

    for block in range(2):
        tab_copy(block).start()
    for c in range(CHANNELS):
        proof_copy(c).start()
    for block in range(2, 8):
        tab_copy(block).start()
    small = [
        pltpu.make_async_copy(target_hbm, target, small_sem.at[0]),
        pltpu.make_async_copy(ttab_hbm, ttab, small_sem.at[1]),
    ]
    for copy in small:
        copy.start()

    for other in OTHERS:
        for cls in range(2):
            pl.semaphore_signal(
                barrier, inc=1, device_id=place(cls, other // 2, other % 2), device_id_type=MESH
            )
    tab_copy(0).wait()
    tab_copy(1).wait()

    def spectra(begin, end, channels):
        lines = tab[begin:end].reshape((end - begin) * 64, 512)
        for c in channels:
            got = nt(lines, proof[c])
            start = c * STRIDE + begin * 64
            stage[0, start : start + (end - begin) * 64, :] = got[:, :128]
            stage[1, start : start + (end - begin) * 64, :] = got[:, 128:]

    def turn(block):
        def one(n, carry):
            for i in range(4):
                row = block * 64 + n * 4 + i
                low = stage[0, pl.ds(row, CHANNELS, stride=STRIDE), :]
                high = stage[1, pl.ds(row, CHANNELS, stride=STRIDE), :]
                xsend[row, :, 0:128] = low.astype(jnp.bfloat16)
                xsend[row, :, 128:256] = high.astype(jnp.bfloat16)
            return carry

        lax.fori_loop(0, POSITIONS, one, 0, unroll=4)

    def send_pair(offset, classes=(0, 1)):
        slot = 3 - offset
        base = [(slot * 2 + cls) * 64 for cls in range(2)]
        for other in OTHERS:
            for cls in classes:
                pltpu.make_async_remote_copy(
                    src_ref=xsend.at[pl.ds(base[cls] + pos_at(cls, other) * 4, 4)],
                    dst_ref=xrecv.at[cls, slot, :, mine[cls]],
                    send_sem=x_send_sem.at[cls, slot],
                    recv_sem=x_recv_sem.at[cls, slot],
                    device_id=place(cls, other // 2, other % 2),
                    device_id_type=MESH,
                ).start()
        for cls in classes:
            for i in range(4):
                xrecv[cls, slot, i, mine[cls]] = xsend[base[cls] + mine[cls] * 4 + i]

    def send_last(offset, classes=(0, 1)):
        slot = 1 - offset
        base = [
            (6 + cls) * 64 + flipped(group[cls][2], offset) * 2 for cls in range(2)
        ]
        for other in OTHERS:
            for cls in classes:
                pltpu.make_async_remote_copy(
                    src_ref=xsend.at[pl.ds(base[cls] + pos_at(cls, other) * 4, 2)],
                    dst_ref=xlast.at[cls, slot, :, mine[cls]],
                    send_sem=x_send_sem.at[cls, 3 + slot],
                    recv_sem=x_recv_sem.at[cls, 3 + slot],
                    device_id=place(cls, other // 2, other % 2),
                    device_id_type=MESH,
                ).start()
        for cls in classes:
            for i in range(2):
                xlast[cls, slot, i, mine[cls]] = xsend[base[cls] + mine[cls] * 4 + i]

    def wait_bytes(view, sem):
        pltpu.make_async_copy(view, view, sem).wait()

    for c in range(8):
        proof_copy(c).wait()
    spectra(0, 2, range(8))
    for c in range(8, CHANNELS):
        proof_copy(c).wait()
    spectra(0, 2, range(8, CHANNELS))
    turn(0)
    turn(1)
    pl.semaphore_wait(barrier, 2 * len(OTHERS))
    send_pair(3)
    for block in range(2, 8):
        tab_copy(block).wait()
    spectra(2, 8, range(CHANNELS))
    turn(2)
    turn(3)
    send_pair(2)
    for block in range(4, 8):
        turn(block)

    for copy in small:
        copy.wait()
    rows[...] = nt(ttab[...], target[...])

    def along_positions(src, dst, sems):
        for other in OTHERS:
            pltpu.make_async_remote_copy(
                src_ref=src(pos_at(0, other)),
                dst_ref=dst(mine[0]),
                send_sem=sems.at[0],
                recv_sem=sems.at[1],
                device_id=place(0, other // 2, other % 2),
                device_id_type=MESH,
            ).start()

    def along_groups(src, dst, sems):
        here = number(v)
        for offset in range(1, GROUPS):
            there = number([flipped(bit, offset & (4 >> n)) for n, bit in enumerate(v)])
            pltpu.make_async_remote_copy(
                src_ref=src.at[there],
                dst_ref=dst.at[here],
                send_sem=sems.at[0],
                recv_sem=sems.at[1],
                device_id=place(1, offset),
                device_id_type=MESH,
            ).start()
        dst[here] = src[here]

    for pos in range(POSITIONS):
        for grp in range(GROUPS):
            at = (pos * GROUPS + grp) * 4
            tsend[pos, grp] = rows[at : at + 4, :].astype(jnp.bfloat16)
    along_positions(lambda p: tsend.at[p], lambda p: tpass.at[:, p], t_sem.at[0])
    for grp in range(GROUPS):
        tpass[grp, mine[0]] = tsend[mine[0], grp]

    def gram(re, im):
        re, im = re.reshape(256, 256), im.reshape(256, 256)
        ret, imt = re.T, im.T
        return (nn(ret, re) + nn(imt, im) + (nn(ret, im) - nn(imt, re))) * (1.0 / 256.0)

    def pair_grams(cls, offset):
        slot = 3 - offset
        wait_bytes(xrecv.at[cls, slot, :, pl.ds(0, POSITIONS - 1)], x_recv_sem.at[cls, slot])
        for bit in (1, 0):
            row = flipped(group[cls][2], bit) * 2
            part[cls, offset * 2 + bit] = gram(
                xrecv[cls, slot, row], xrecv[cls, slot, row + 1]
            )

    def last_gram(cls, offset):
        slot = 1 - offset
        wait_bytes(xlast.at[cls, slot, :, pl.ds(0, POSITIONS - 1)], x_recv_sem.at[cls, 3 + slot])
        part[cls, offset] = gram(xlast[cls, slot, 0], xlast[cls, slot, 1])

    def gram_sum(cls, offset, piece):
        total = part[cls, offset, pl.ds(piece * PIECE, PIECE), :]
        for other in feeders(offset, piece):
            wait_bytes(mrecv.at[cls, piece, other], m_recv_sem.at[cls, piece, other])
            total = total + mrecv[cls, piece, other].astype(jnp.float32)
        return total

    def pass_on(cls, offset, piece):
        msend[cls, piece, offset] = gram_sum(cls, offset, piece).astype(jnp.bfloat16)
        pltpu.make_async_remote_copy(
            src_ref=msend.at[cls, piece, offset],
            dst_ref=mrecv.at[cls, piece, offset],
            send_sem=m_send_sem.at[cls, piece, offset],
            recv_sem=m_recv_sem.at[cls, piece, offset],
            device_id=place(1 - cls, next_bit(offset, piece)),
            device_id_type=MESH,
        ).start()

    for cls in range(2):
        pair_grams(cls, 3)
        pass_on(cls, 7, 0)
        pass_on(cls, 7, 1)
        pass_on(cls, 6, 0)
        send_pair(1, (cls,))
    for cls in range(2):
        pair_grams(cls, 2)
        pass_on(cls, 5, 0)
        pass_on(cls, 5, 1)
        pass_on(cls, 4, 0)
        send_last(1, (cls,))
    wait_bytes(tpass.at[:, pl.ds(0, POSITIONS - 1)], t_sem.at[0, 1])
    along_groups(tpass, trecv, t_sem.at[1])
    for cls in range(2):
        pass_on(cls, 6, 1)
    for cls in range(2):
        pair_grams(cls, 1)
        pass_on(cls, 3, 0)
        pass_on(cls, 3, 1)
        pass_on(cls, 2, 0)
        send_last(0, (cls,))
    for cls in range(2):
        pass_on(cls, 4, 1)
    for cls in range(2):
        last_gram(cls, 1)
        pass_on(cls, 1, 0)
        pass_on(cls, 1, 1)
    for cls in range(2):
        pass_on(cls, 2, 1)

    lane = lax.broadcasted_iota(jnp.int32, (16, 128), 1) // 32
    wait_bytes(trecv.at[pl.ds(0, GROUPS - 1)], t_sem.at[1, 1])
    for device in range(128):
        bits_v, bits_u, its_core = split_place(device // 8, device % 8)
        rows[device * 4 : device * 4 + 4, :] = trecv[
            number(bits_v), number(bits_u) * 2 + its_core
        ].astype(jnp.float32)
    for i in range(4):
        blocks = [rows[pl.ds(g * 4 + i, 16, stride=32), :] for g in range(8)]
        for t in range(4):
            for tile in range(2):
                total = jnp.zeros((16, 128), jnp.float32)
                for k in range(4):
                    turned = blocks[tile * 4 + k]
                    if k != t:
                        turned = pltpu.roll(turned, (32 * (k - t)) % 128, 1)
                    total = jnp.where(lane == k, turned, total)
                tmat[
                    i // 2, (i % 2) * 64 + t * 16 : (i % 2) * 64 + t * 16 + 16,
                    tile * 128 : tile * 128 + 128,
                ] = total.astype(jnp.bfloat16)

    for cls in range(2):
        last_gram(cls, 0)

    bins = bins_of(v, u, core)
    for cls in range(2):
        total = jnp.concatenate([gram_sum(cls, 0, piece) for piece in range(2)], axis=0)
        high = total.astype(jnp.bfloat16)
        low = (total - high.astype(jnp.float32)).astype(jnp.bfloat16)

        def combine(straight, turned):
            return (
                0.5 * (straight[:64] - straight[64:] + turned[:64] + turned[64:]),
                0.5 * (straight[:64] + straight[64:] - turned[:64] + turned[64:]),
            )

        left = tmat[cls]
        once_re, once_im = combine(
            nn(left, high) + nn(left, low), nt(left, high) + nt(left, low)
        )
        once = jnp.concatenate([once_re, once_im], axis=0)
        once_high = once.astype(jnp.bfloat16)
        once_low = (once - once_high.astype(jnp.float32)).astype(jnp.bfloat16)
        both = jnp.concatenate([once_high, once_low], axis=0)
        straight, turned = nn(both, high), nt(both, high)
        twice_re, twice_im = combine(
            straight[:128] + straight[128:] + nn(once_high, low),
            turned[:128] + turned[128:] + nt(once_high, low),
        )
        load = loading[bins[cls]]
        step = 1.0 / (load + rho)
        keep, take = 2.0 * step - load * step * step, step * step
        pred = (keep * once_re - take * twice_re, keep * once_im - take * twice_im)
        for side in range(2):
            for g in range(8):
                k, tile = g % 4, g // 4
                moved = jnp.zeros((16, 128), jnp.float32)
                for t in range(4):
                    turned = pred[side][t * 16 : t * 16 + 16, tile * 128 : tile * 128 + 128]
                    if k != t:
                        turned = pltpu.roll(turned, (32 * (t - k)) % 128, 1)
                    moved = jnp.where(lane == t, turned, moved)
                rows[pl.ds(g * 4 + cls * 2 + side, 16, stride=32), :] = moved

    me = gx * 8 + gy
    for device in range(128):
        psend[device] = rows[device * 4 : device * 4 + 4, :].astype(jnp.bfloat16)
    columns = [(gy + n) % 8 for n in range(8)]

    def give(row, column):
        pltpu.make_async_remote_copy(
            src_ref=psend.at[row * 8 + column],
            dst_ref=precv.at[me],
            send_sem=p_sem.at[0],
            recv_sem=p_sem.at[1],
            device_id=(row, column),
            device_id_type=MESH,
        ).start()

    def give_line(n, carry):
        for column in columns:
            give((gx + n) % 16, column)
        return carry

    lax.fori_loop(1, 16, give_line, 0)
    for column in columns[1:]:
        give(gx, column)
    precv[me] = psend[me]
    wait_bytes(precv.at[pl.ds(0, 127)], p_sem.at[1])
    for device in range(128):
        rows[device * 4 : device * 4 + 4, :] = precv[device].astype(jnp.float32)
    out[...] = rows[...].astype(jnp.bfloat16)

    for cls in range(2):
        for slot in range(3):
            wait_bytes(xrecv.at[cls, slot, :, pl.ds(0, POSITIONS - 1)], x_send_sem.at[cls, slot])
        for slot in range(2):
            wait_bytes(xlast.at[cls, slot, :, pl.ds(0, POSITIONS - 1)], x_send_sem.at[cls, 3 + slot])
        for piece in range(2):
            for offset in range(1, GROUPS):
                wait_bytes(msend.at[cls, piece, offset], m_send_sem.at[cls, piece, offset])
    wait_bytes(tpass.at[:, pl.ds(0, POSITIONS - 1)], t_sem.at[0, 0])
    wait_bytes(trecv.at[pl.ds(0, GROUPS - 1)], t_sem.at[1, 0])
    wait_bytes(precv.at[pl.ds(0, 127)], p_sem.at[0])


def tables(length):
    forward, inverse = transform_tables(length)
    by_pair = (
        forward.reshape(2, POSITIONS, 4, 4, length)
        .transpose(0, 2, 1, 3, 4)
        .reshape(8, POSITIONS * 4, length)
    )
    first = []
    bits = [(n // 4, n // 2 % 2, n % 2) for n in range(GROUPS)]
    for pos in range(POSITIONS):
        for grp in range(GROUPS):
            for found in bins_of(bits[grp], bits[pos // 2], pos % 2):
                first += [2 * found, 2 * found + 1]
    second = []
    for device in range(128):
        for found in bins_of(*split_place(device // 8, device % 8)):
            second += [2 * found, 2 * found + 1]
    return tuple(
        jnp.asarray(table).astype(jnp.bfloat16)
        for table in (by_pair, forward[first], inverse[second])
    )


def local(proof, target, loading):
    channels, segments, length = proof.shape
    rho = (1.0 + math.sqrt(2048 / segments)) ** 2
    by_pair, by_owner, inverse = tables(length)
    bf16, f32 = jnp.bfloat16, jnp.float32
    hbm = pl.BlockSpec(memory_space=pltpu.HBM)
    scratch = [
        pltpu.VMEM((8, 64, 512), bf16),
        pltpu.VMEM((512, 512), bf16),
        pltpu.VMEM((16, 256, 512), bf16),
        pltpu.VMEM((128, 512), bf16),
        pltpu.VMEM((2, CHANNELS * STRIDE, 128), f32),
        pltpu.VMEM((512, CHANNELS, 256), bf16),
        pltpu.VMEM((2, 3, 4, POSITIONS, CHANNELS, 256), bf16),
        pltpu.VMEM((2, 2, 2, POSITIONS, CHANNELS, 256), bf16),
        pltpu.VMEM((2, GROUPS, 256, 256), f32),
        pltpu.VMEM((2, 2, GROUPS, PIECE, 256), bf16),
        pltpu.VMEM((2, 2, GROUPS, PIECE, 256), bf16),
        pltpu.VMEM((2, 128, 256), bf16),
        pltpu.VMEM((POSITIONS, GROUPS, 4, 128), bf16),
        pltpu.VMEM((GROUPS, POSITIONS, 4, 128), bf16),
        pltpu.VMEM((GROUPS, POSITIONS, 4, 128), bf16),
        pltpu.VMEM((512, 128), f32),
        pltpu.VMEM((128, 4, 128), bf16),
        pltpu.VMEM((128, 4, 128), bf16),
        pltpu.SemaphoreType.DMA((CHANNELS,)),
        pltpu.SemaphoreType.DMA((8,)),
        pltpu.SemaphoreType.DMA((2,)),
        pltpu.SemaphoreType.DMA((2, 5)),
        pltpu.SemaphoreType.DMA((2, 5)),
        pltpu.SemaphoreType.DMA((2, 2, GROUPS)),
        pltpu.SemaphoreType.DMA((2, 2, GROUPS)),
        pltpu.SemaphoreType.DMA((2, 2)),
        pltpu.SemaphoreType.DMA((2,)),
    ]
    hold = [
        pltpu.with_memory_space_constraint(array, pltpu.HBM)
        for array in (by_pair, by_owner, proof, target.reshape(128, length))
    ]
    spectra = pl.pallas_call(
        functools.partial(kernel, rho),
        out_shape=jax.ShapeDtypeStruct((512, 128), bf16),
        in_specs=[hbm] * 4 + [pl.BlockSpec(memory_space=pltpu.SMEM)],
        out_specs=pl.BlockSpec(memory_space=pltpu.VMEM),
        scratch_shapes=scratch,
        compiler_params=pltpu.CompilerParams(
            collective_id=0, has_side_effects=True, vmem_limit_bytes=40 * 2**20
        ),
    )(*hold, loading)
    return tn(spectra, inverse).reshape(4, 32, length)


def solution(mesh):
    return jax.shard_map(
        local,
        mesh=mesh,
        in_specs=(P(("gx", "gy"), None, None), P("gx", "gy", None), P()),
        out_specs=P("gx", "gy", None),
        check_vma=False,
    )
```

```python
import functools
import math

import jax
import jax.numpy as jnp
import numpy as np
from jax import lax
from jax.experimental import pallas as pl
from jax.experimental.pallas import tpu as pltpu
from jax.sharding import PartitionSpec as P

GROUPS = 8
POSITIONS = 16
CHANNELS = 16
STRIDE = 520
OTHERS = (2, 4, 8, 14, 3, 5, 9, 15, 6, 12, 10, 7, 13, 11, 1)
FAR_FIRST = sorted(
    ((v, u, core) for v in range(8) for u in range(8) for core in range(2) if v or u or core),
    key=lambda way: -(way[0].bit_count() + way[1].bit_count()),
)
PIECE = 128
ORDERS = ((2, 4, 1), (1, 4, 2))
MESH = pl.DeviceIdType.MESH


def transform_tables(length):
    half = length // 2
    sample = np.arange(length)
    phase = ((np.arange(half)[:, None] * sample[None, :]) % length).astype(np.float32) * np.float32(
        2.0 * math.pi / length
    )
    angle = sample.astype(np.float32) * np.float32(2.0 * math.pi / length)
    window = np.float32(0.5) - np.float32(0.5) * np.cos(angle)
    forward = np.stack([window * np.cos(phase), -window * np.sin(phase)], axis=1).reshape(
        length, length
    ) * np.float32(1.0 / math.sqrt(0.375 * length))
    inverse = np.stack([np.cos(phase), -np.sin(phase)], axis=1).reshape(
        length, length
    ) * np.float32(math.sqrt(2.0 / length))
    return forward.astype(np.float32), inverse.astype(np.float32)


def split_place(gx, gy):
    core, z, yh = gx % 2, (gx // 2) % 4, gx // 8
    x, yl = gy % 4, gy // 4
    v = (z // 2, yh, x // 2)
    return v, ((z + v[0]) % 2, (yl + yh) % 2, (x + v[2]) % 2), core


def number(bits):
    return (bits[0] * 2 + bits[1]) * 2 + bits[2]


def bins_of(v, u, core):
    return (
        (number(u) * 2 + core) * GROUPS + number(v),
        128 + (number(v) * 2 + core) * GROUPS + number(u),
    )


def next_bit(offset, piece):
    return next(bit for bit in ORDERS[piece] if offset & bit)


def feeders(offset, piece):
    return [
        other for other in range(1, GROUPS) if other ^ next_bit(other, piece) == offset
    ]


def nt(left, right):
    return lax.dot_general(
        left, right, (((1,), (1,)), ((), ())), preferred_element_type=jnp.float32
    )


def nn(left, right):
    return lax.dot_general(
        left, right, (((1,), (0,)), ((), ())), preferred_element_type=jnp.float32
    )


def tn(left, right):
    return lax.dot_general(
        left, right, (((0,), (0,)), ((), ())), preferred_element_type=jnp.float32
    )


def kernel(
    rho,
    tab_hbm, ttab_hbm, proof_hbm, target_hbm, loading_hbm,
    out,
    tab, ttab, proof, target, loading,
    stage, xsend, xrecv, xlast, part, msend, mrecv, tmat, tsend, tpass, trecv, rows, psend, precv,
    proof_sem, tab_sem, small_sem,
    x_send_sem, x_recv_sem, m_send_sem, m_recv_sem, t_sem, p_sem,
):
    gx, gy = lax.axis_index("gx"), lax.axis_index("gy")
    v, u, core = split_place(gx, gy)
    group = (v, u)
    mine = (number(u) * 2 + core, number(v) * 2 + core)

    z, yh, x, yl = (gx // 2) % 4, gx // 8, gy % 4, gy // 4
    z_flip = (2 * v[0] + 1 - z % 2, 2 * (1 - v[0]) + 1 - z % 2, 2 * (1 - v[0]) + z % 2)
    x_flip = (2 * v[2] + 1 - x % 2, 2 * (1 - v[2]) + 1 - x % 2, 2 * (1 - v[2]) + x % 2)

    def place_off(by_v, by_u, flip_core=0):
        turns_z = (z, z_flip[0], z_flip[1], z_flip[2])
        turns_x = (x, x_flip[0], x_flip[1], x_flip[2])
        there_z = turns_z[(by_v >> 2 & 1) * 2 + (by_u >> 2 & 1)]
        there_x = turns_x[(by_v & 1) * 2 + (by_u & 1)]
        there_yh = 1 - yh if by_v & 2 else yh
        there_yl = 1 - yl if (by_v ^ by_u) & 2 else yl
        there_core = 1 - core if flip_core else core
        return there_yh * 8 + there_z * 2 + there_core, there_yl * 4 + there_x

    def place(which, offset, flip_core=0):
        return place_off(*((0, offset) if which == 0 else (offset, 0)), flip_core)

    def flipped(bit, flip):
        return 1 - bit if flip else bit

    def pos_at(cls, offset):
        bits = (u, v)[cls]
        return (
            number([flipped(b, offset & (8 >> n)) for n, b in enumerate(bits)]) * 2
            + flipped(core, offset & 1)
        )

    def pair_at(cls, offset):
        bits = group[cls]
        return flipped(bits[0], offset & 2) * 2 + flipped(bits[1], offset & 1)

    barrier = pltpu.get_barrier_semaphore()

    def tab_copy(block):
        cls, offset = block % 2, 3 - block // 2
        return pltpu.make_async_copy(
            tab_hbm.at[cls * 4 + pair_at(cls, offset)], tab.at[block], tab_sem.at[block]
        )

    def proof_copy(c):
        return pltpu.make_async_copy(proof_hbm.at[c], proof.at[c], proof_sem.at[c])

    for block in range(2):
        tab_copy(block).start()
    for c in range(CHANNELS):
        proof_copy(c).start()
    for block in range(2, 8):
        tab_copy(block).start()
    small = [
        pltpu.make_async_copy(target_hbm, target, small_sem.at[0]),
        pltpu.make_async_copy(ttab_hbm, ttab, small_sem.at[1]),
        pltpu.make_async_copy(loading_hbm, loading, small_sem.at[2]),
    ]
    for copy in small:
        copy.start()

    for other in OTHERS:
        for cls in range(2):
            pl.semaphore_signal(
                barrier, inc=1, device_id=place(cls, other // 2, other % 2), device_id_type=MESH
            )
    tab_copy(0).wait()
    tab_copy(1).wait()

    def spectra(begin, end, channels):
        lines = tab[begin:end].reshape((end - begin) * 64, 512)
        for c in channels:
            got = nt(lines, proof[c])
            start = c * STRIDE + begin * 64
            stage[0, start : start + (end - begin) * 64, :] = got[:, :128]
            stage[1, start : start + (end - begin) * 64, :] = got[:, 128:]

    def turn(block):
        def one(n, carry):
            for i in range(4):
                row = block * 64 + n * 4 + i
                low = stage[0, pl.ds(row, CHANNELS, stride=STRIDE), :]
                high = stage[1, pl.ds(row, CHANNELS, stride=STRIDE), :]
                xsend[row, :, 0:128] = low.astype(jnp.bfloat16)
                xsend[row, :, 128:256] = high.astype(jnp.bfloat16)
            return carry

        lax.fori_loop(0, POSITIONS, one, 0, unroll=4)

    def send_pair(offset, classes=(0, 1)):
        slot = 3 - offset
        base = [(slot * 2 + cls) * 64 for cls in range(2)]
        for other in OTHERS:
            for cls in classes:
                pltpu.make_async_remote_copy(
                    src_ref=xsend.at[pl.ds(base[cls] + pos_at(cls, other) * 4, 4)],
                    dst_ref=xrecv.at[cls, slot, :, mine[cls]],
                    send_sem=x_send_sem.at[cls, slot],
                    recv_sem=x_recv_sem.at[cls, slot],
                    device_id=place(cls, other // 2, other % 2),
                    device_id_type=MESH,
                ).start()
        for cls in classes:
            for i in range(4):
                xrecv[cls, slot, i, mine[cls]] = xsend[base[cls] + mine[cls] * 4 + i]

    def send_single(offset, classes=(0, 1)):
        slot = 3 - offset
        base = [
            ((3 - offset // 2) * 2 + cls) * 64 + flipped(group[cls][2], offset % 2) * 2
            for cls in range(2)
        ]
        for other in OTHERS:
            for cls in classes:
                pltpu.make_async_remote_copy(
                    src_ref=xsend.at[pl.ds(base[cls] + pos_at(cls, other) * 4, 2)],
                    dst_ref=xlast.at[cls, slot, :, mine[cls]],
                    send_sem=x_send_sem.at[cls, 2 + slot],
                    recv_sem=x_recv_sem.at[cls, 2 + slot],
                    device_id=place(cls, other // 2, other % 2),
                    device_id_type=MESH,
                ).start()
        for cls in classes:
            for i in range(2):
                xlast[cls, slot, i, mine[cls]] = xsend[base[cls] + mine[cls] * 4 + i]

    def wait_bytes(view, sem):
        pltpu.make_async_copy(view, view, sem).wait()

    def along_positions(src, dst, sems):
        for other in OTHERS:
            pltpu.make_async_remote_copy(
                src_ref=src(pos_at(0, other)),
                dst_ref=dst(mine[0]),
                send_sem=sems.at[0],
                recv_sem=sems.at[1],
                device_id=place(0, other // 2, other % 2),
                device_id_type=MESH,
            ).start()

    def along_groups(src, dst, sems):
        here = number(v)
        for offset in range(1, GROUPS):
            there = number([flipped(bit, offset & (4 >> n)) for n, bit in enumerate(v)])
            pltpu.make_async_remote_copy(
                src_ref=src.at[there],
                dst_ref=dst.at[here],
                send_sem=sems.at[0],
                recv_sem=sems.at[1],
                device_id=place(1, offset),
                device_id_type=MESH,
            ).start()
        dst[here] = src[here]

    for begin, end in ((0, 4), (4, 8), (8, CHANNELS)):
        for c in range(begin, end):
            proof_copy(c).wait()
        spectra(0, 2, range(begin, end))
    turn(0)
    pl.semaphore_wait(barrier, 2 * len(OTHERS))
    send_pair(3, (0,))
    turn(1)
    send_pair(3, (1,))
    for block in range(2, 8):
        tab_copy(block).wait()
    spectra(2, 8, range(CHANNELS))
    turn(2)
    turn(3)
    send_pair(2)
    turn(4)
    turn(5)
    for copy in small:
        copy.wait()
    rows[...] = nt(ttab[...], target[...])

    for pos in range(POSITIONS):
        for grp in range(GROUPS):
            at = (pos * GROUPS + grp) * 4
            tsend[pos, grp] = rows[at : at + 4, :].astype(jnp.bfloat16)
    along_positions(lambda p: tsend.at[p], lambda p: tpass.at[:, p], t_sem.at[0])
    for grp in range(GROUPS):
        tpass[grp, mine[0]] = tsend[mine[0], grp]

    send_single(3)
    turn(6)
    turn(7)

    def gram(re, im):
        re, im = re.reshape(256, 256), im.reshape(256, 256)
        ret, imt = re.T, im.T
        return (nn(ret, re) + nn(imt, im) + (nn(ret, im) - nn(imt, re))) * (1.0 / 256.0)

    def pair_grams(cls, offset):
        slot = 3 - offset
        wait_bytes(xrecv.at[cls, slot, :, pl.ds(0, POSITIONS - 1)], x_recv_sem.at[cls, slot])
        for bit in (1, 0):
            row = flipped(group[cls][2], bit) * 2
            part[cls, offset * 2 + bit] = gram(
                xrecv[cls, slot, row], xrecv[cls, slot, row + 1]
            )

    def single_gram(cls, offset):
        slot = 3 - offset
        wait_bytes(xlast.at[cls, slot, :, pl.ds(0, POSITIONS - 1)], x_recv_sem.at[cls, 2 + slot])
        part[cls, offset] = gram(xlast[cls, slot, 0], xlast[cls, slot, 1])

    def wait_fed(cls, offset, piece):
        for other in feeders(offset, piece):
            wait_bytes(mrecv.at[cls, piece, other], m_recv_sem.at[cls, piece, other])

    def wait_sums(offset):
        for cls in range(2):
            for piece in range(2):
                wait_fed(cls, offset, piece)

    def gram_sum(cls, offset, piece):
        total = part[cls, offset, pl.ds(piece * PIECE, PIECE), :]
        for other in feeders(offset, piece):
            total = total + mrecv[cls, piece, other].astype(jnp.float32)
        return total

    def pass_on(cls, offset, piece):
        wait_fed(cls, offset, piece)
        msend[cls, piece, offset] = gram_sum(cls, offset, piece).astype(jnp.bfloat16)
        pltpu.make_async_remote_copy(
            src_ref=msend.at[cls, piece, offset],
            dst_ref=mrecv.at[cls, piece, offset],
            send_sem=m_send_sem.at[cls, piece, offset],
            recv_sem=m_recv_sem.at[cls, piece, offset],
            device_id=place(1 - cls, next_bit(offset, piece)),
            device_id_type=MESH,
        ).start()

    for cls in range(2):
        pair_grams(cls, 3)
        pass_on(cls, 7, 1)
        pass_on(cls, 7, 0)
        pass_on(cls, 6, 0)
    send_single(2)
    for cls in range(2):
        pair_grams(cls, 2)
        pass_on(cls, 5, 1)
    send_single(1)
    wait_bytes(tpass.at[:, pl.ds(0, POSITIONS - 1)], t_sem.at[0, 1])
    along_groups(tpass, trecv, t_sem.at[1])
    for cls in range(2):
        pass_on(cls, 6, 1)
    for cls in range(2):
        pass_on(cls, 5, 0)
        pass_on(cls, 4, 0)
    for cls in range(2):
        single_gram(cls, 3)
        single_gram(cls, 2)
        pass_on(cls, 3, 1)
        pass_on(cls, 3, 0)
        pass_on(cls, 2, 0)
    send_single(0)
    for cls in range(2):
        pass_on(cls, 4, 1)
    for cls in range(2):
        single_gram(cls, 1)
        pass_on(cls, 1, 1)
        pass_on(cls, 1, 0)
    for cls in range(2):
        pass_on(cls, 2, 1)

    lane = lax.broadcasted_iota(jnp.int32, (16, 128), 1) // 32
    wait_bytes(trecv.at[pl.ds(0, GROUPS - 1)], t_sem.at[1, 1])
    for device in range(128):
        bits_v, bits_u, its_core = split_place(device // 8, device % 8)
        rows[device * 4 : device * 4 + 4, :] = trecv[
            number(bits_v), number(bits_u) * 2 + its_core
        ].astype(jnp.float32)
    for i in range(4):
        blocks = [rows[pl.ds(g * 4 + i, 16, stride=32), :] for g in range(8)]
        for t in range(4):
            for tile in range(2):
                total = jnp.zeros((16, 128), jnp.float32)
                for k in range(4):
                    turned = blocks[tile * 4 + k]
                    if k != t:
                        turned = pltpu.roll(turned, (32 * (k - t)) % 128, 1)
                    total = jnp.where(lane == k, turned, total)
                tmat[
                    i // 2, (i % 2) * 64 + t * 16 : (i % 2) * 64 + t * 16 + 16,
                    tile * 128 : tile * 128 + 128,
                ] = total.astype(jnp.bfloat16)

    for cls in range(2):
        single_gram(cls, 0)

    bins = bins_of(v, u, core)

    def combine(straight, turned):
        return (
            0.5 * (straight[:64] - straight[64:] + turned[:64] + turned[64:]),
            0.5 * (straight[:64] + straight[64:] - turned[:64] + turned[64:]),
        )

    def halves(whole):
        high = whole.astype(jnp.bfloat16)
        return high, (whole - high.astype(jnp.float32)).astype(jnp.bfloat16)

    wait_sums(0)
    both_grams = [
        halves(jnp.concatenate([gram_sum(cls, 0, piece) for piece in range(2)], axis=0))
        for cls in range(2)
    ]
    both_once = []
    for cls in range(2):
        (high, low), left = both_grams[cls], tmat[cls]
        both_once.append(
            combine(nn(left, high) + nn(left, low), nt(left, high) + nt(left, low))
        )
    both_twice = []
    for cls in range(2):
        high, low = both_grams[cls]
        once_high, once_low = halves(jnp.concatenate(both_once[cls], axis=0))
        lines = jnp.concatenate([once_high, once_low], axis=0)
        straight, turned = nn(lines, high), nt(lines, high)
        both_twice.append(
            combine(
                straight[:128] + straight[128:] + nn(once_high, low),
                turned[:128] + turned[128:] + nt(once_high, low),
            )
        )
    for cls in range(2):
        load = loading[bins[cls]]
        step = 1.0 / (load + rho)
        keep, take = 2.0 * step - load * step * step, step * step
        for side in range(2):
            pred = keep * both_once[cls][side] - take * both_twice[cls][side]
            for g in range(8):
                k, tile = g % 4, g // 4
                moved = jnp.zeros((16, 128), jnp.float32)
                for t in range(4):
                    turned = pred[t * 16 : t * 16 + 16, tile * 128 : tile * 128 + 128]
                    if k != t:
                        turned = pltpu.roll(turned, (32 * (t - k)) % 128, 1)
                    moved = jnp.where(lane == t, turned, moved)
                rows[pl.ds(g * 4 + cls * 2 + side, 16, stride=32), :] = moved

    me = gx * 8 + gy
    for device in range(128):
        psend[device] = rows[device * 4 : device * 4 + 4, :].astype(jnp.bfloat16)
    for by_v, by_u, flip_core in FAR_FIRST:
        row, column = place_off(by_v, by_u, flip_core)
        pltpu.make_async_remote_copy(
            src_ref=psend.at[row * 8 + column],
            dst_ref=precv.at[me],
            send_sem=p_sem.at[0],
            recv_sem=p_sem.at[1],
            device_id=(row, column),
            device_id_type=MESH,
        ).start()
    precv[me] = psend[me]
    wait_bytes(precv.at[pl.ds(0, 127)], p_sem.at[1])
    for device in range(128):
        rows[device * 4 : device * 4 + 4, :] = precv[device].astype(jnp.float32)
    out[...] = rows[...].astype(jnp.bfloat16)

    for cls in range(2):
        for slot in range(2):
            wait_bytes(xrecv.at[cls, slot, :, pl.ds(0, POSITIONS - 1)], x_send_sem.at[cls, slot])
        for slot in range(4):
            wait_bytes(xlast.at[cls, slot, :, pl.ds(0, POSITIONS - 1)], x_send_sem.at[cls, 2 + slot])
        for piece in range(2):
            for offset in range(1, GROUPS):
                wait_bytes(msend.at[cls, piece, offset], m_send_sem.at[cls, piece, offset])
    wait_bytes(tpass.at[:, pl.ds(0, POSITIONS - 1)], t_sem.at[0, 0])
    wait_bytes(trecv.at[pl.ds(0, GROUPS - 1)], t_sem.at[1, 0])
    wait_bytes(precv.at[pl.ds(0, 127)], p_sem.at[0])


def tables(length):
    forward, inverse = transform_tables(length)
    by_pair = (
        forward.reshape(2, POSITIONS, 4, 4, length)
        .transpose(0, 2, 1, 3, 4)
        .reshape(8, POSITIONS * 4, length)
    )
    first = []
    bits = [(n // 4, n // 2 % 2, n % 2) for n in range(GROUPS)]
    for pos in range(POSITIONS):
        for grp in range(GROUPS):
            for found in bins_of(bits[grp], bits[pos // 2], pos % 2):
                first += [2 * found, 2 * found + 1]
    second = []
    for device in range(128):
        for found in bins_of(*split_place(device // 8, device % 8)):
            second += [2 * found, 2 * found + 1]
    return tuple(
        jnp.asarray(table).astype(jnp.bfloat16)
        for table in (by_pair, forward[first], inverse[second])
    )


def local(proof, target, loading):
    channels, segments, length = proof.shape
    rho = (1.0 + math.sqrt(2048 / segments)) ** 2
    by_pair, by_owner, inverse = tables(length)
    bf16, f32 = jnp.bfloat16, jnp.float32
    hbm = pl.BlockSpec(memory_space=pltpu.HBM)
    scratch = [
        pltpu.VMEM((8, 64, 512), bf16),
        pltpu.VMEM((512, 512), bf16),
        pltpu.VMEM((16, 256, 512), bf16),
        pltpu.VMEM((128, 512), bf16),
        pltpu.SMEM((256,), f32),
        pltpu.VMEM((2, CHANNELS * STRIDE, 128), f32),
        pltpu.VMEM((512, CHANNELS, 256), bf16),
        pltpu.VMEM((2, 2, 4, POSITIONS, CHANNELS, 256), bf16),
        pltpu.VMEM((2, 4, 2, POSITIONS, CHANNELS, 256), bf16),
        pltpu.VMEM((2, GROUPS, 256, 256), f32),
        pltpu.VMEM((2, 2, GROUPS, PIECE, 256), bf16),
        pltpu.VMEM((2, 2, GROUPS, PIECE, 256), bf16),
        pltpu.VMEM((2, 128, 256), bf16),
        pltpu.VMEM((POSITIONS, GROUPS, 4, 128), bf16),
        pltpu.VMEM((GROUPS, POSITIONS, 4, 128), bf16),
        pltpu.VMEM((GROUPS, POSITIONS, 4, 128), bf16),
        pltpu.VMEM((512, 128), f32),
        pltpu.VMEM((128, 4, 128), bf16),
        pltpu.VMEM((128, 4, 128), bf16),
        pltpu.SemaphoreType.DMA((CHANNELS,)),
        pltpu.SemaphoreType.DMA((8,)),
        pltpu.SemaphoreType.DMA((3,)),
        pltpu.SemaphoreType.DMA((2, 6)),
        pltpu.SemaphoreType.DMA((2, 6)),
        pltpu.SemaphoreType.DMA((2, 2, GROUPS)),
        pltpu.SemaphoreType.DMA((2, 2, GROUPS)),
        pltpu.SemaphoreType.DMA((2, 2)),
        pltpu.SemaphoreType.DMA((2,)),
    ]
    hold = [
        pltpu.with_memory_space_constraint(array, pltpu.HBM)
        for array in (by_pair, by_owner, proof, target.reshape(128, length), loading)
    ]
    spectra = pl.pallas_call(
        functools.partial(kernel, rho),
        out_shape=jax.ShapeDtypeStruct((512, 128), bf16),
        in_specs=[hbm] * 5,
        out_specs=pl.BlockSpec(memory_space=pltpu.VMEM),
        scratch_shapes=scratch,
        compiler_params=pltpu.CompilerParams(
            collective_id=0, has_side_effects=True, vmem_limit_bytes=40 * 2**20
        ),
    )(*hold)
    return tn(spectra, inverse).reshape(4, 32, length)


def solution(mesh):
    return jax.shard_map(
        local,
        mesh=mesh,
        in_specs=(P(("gx", "gy"), None, None), P("gx", "gy", None), P()),
        out_specs=P("gx", "gy", None),
        check_vma=False,
    )
```

```python
import functools
import math

import jax
import jax.numpy as jnp
import numpy as np
from jax import lax
from jax.experimental import pallas as pl
from jax.experimental.pallas import tpu as pltpu
from jax.sharding import PartitionSpec as P

GROUPS = 8
POSITIONS = 16
CHANNELS = 16
STRIDE = 520
OTHERS = (14, 12, 6, 10, 8, 4, 2, 15, 13, 7, 11, 9, 5, 3, 1)
FAR_FIRST = sorted(
    ((v, u, core) for v in range(8) for u in range(8) for core in range(2) if v or u or core),
    key=lambda way: -(way[0].bit_count() + way[1].bit_count()),
)
PIECE = 128
ORDERS = ((2, 4, 1), (1, 4, 2))
MESH = pl.DeviceIdType.MESH


def transform_tables(length):
    half = length // 2
    sample = np.arange(length)
    phase = ((np.arange(half)[:, None] * sample[None, :]) % length).astype(np.float32) * np.float32(
        2.0 * math.pi / length
    )
    angle = sample.astype(np.float32) * np.float32(2.0 * math.pi / length)
    window = np.float32(0.5) - np.float32(0.5) * np.cos(angle)
    forward = np.stack([window * np.cos(phase), -window * np.sin(phase)], axis=1).reshape(
        length, length
    ) * np.float32(1.0 / math.sqrt(0.375 * length))
    inverse = np.stack([np.cos(phase), -np.sin(phase)], axis=1).reshape(
        length, length
    ) * np.float32(math.sqrt(2.0 / length))
    return forward.astype(np.float32), inverse.astype(np.float32)


def split_place(gx, gy):
    core, z, yh = gx % 2, (gx // 2) % 4, gx // 8
    x, yl = gy % 4, gy // 4
    v = (z // 2, yh, x // 2)
    return v, ((z + v[0]) % 2, (yl + yh) % 2, (x + v[2]) % 2), core


def number(bits):
    return (bits[0] * 2 + bits[1]) * 2 + bits[2]


def bins_of(v, u, core):
    return (
        (number(u) * 2 + core) * GROUPS + number(v),
        128 + (number(v) * 2 + core) * GROUPS + number(u),
    )


def next_bit(offset, piece):
    return next(bit for bit in ORDERS[piece] if offset & bit)


def feeders(offset, piece):
    return [
        other for other in range(1, GROUPS) if other ^ next_bit(other, piece) == offset
    ]


def nt(left, right):
    return lax.dot_general(
        left, right, (((1,), (1,)), ((), ())), preferred_element_type=jnp.float32
    )


def nn(left, right):
    return lax.dot_general(
        left, right, (((1,), (0,)), ((), ())), preferred_element_type=jnp.float32
    )


def tn(left, right):
    return lax.dot_general(
        left, right, (((0,), (0,)), ((), ())), preferred_element_type=jnp.float32
    )


def kernel(
    rho,
    tab_hbm, ttab_hbm, proof_hbm, target_hbm, loading_hbm,
    out,
    tab, ttab, proof, target, loading,
    stage, xsend, xrecv, xlast, part, msend, mrecv, tmat, tsend, tpass, trecv, rows, psend, precv,
    proof_sem, tab_sem, small_sem,
    x_send_sem, x_recv_sem, m_send_sem, m_recv_sem, t_sem, p_sem,
):
    gx, gy = lax.axis_index("gx"), lax.axis_index("gy")
    v, u, core = split_place(gx, gy)
    group = (v, u)
    mine = (number(u) * 2 + core, number(v) * 2 + core)

    z, yh, x, yl = (gx // 2) % 4, gx // 8, gy % 4, gy // 4
    z_flip = (2 * v[0] + 1 - z % 2, 2 * (1 - v[0]) + 1 - z % 2, 2 * (1 - v[0]) + z % 2)
    x_flip = (2 * v[2] + 1 - x % 2, 2 * (1 - v[2]) + 1 - x % 2, 2 * (1 - v[2]) + x % 2)

    def place_off(by_v, by_u, flip_core=0):
        turns_z = (z, z_flip[0], z_flip[1], z_flip[2])
        turns_x = (x, x_flip[0], x_flip[1], x_flip[2])
        there_z = turns_z[(by_v >> 2 & 1) * 2 + (by_u >> 2 & 1)]
        there_x = turns_x[(by_v & 1) * 2 + (by_u & 1)]
        there_yh = 1 - yh if by_v & 2 else yh
        there_yl = 1 - yl if (by_v ^ by_u) & 2 else yl
        there_core = 1 - core if flip_core else core
        return there_yh * 8 + there_z * 2 + there_core, there_yl * 4 + there_x

    def place(which, offset, flip_core=0):
        return place_off(*((0, offset) if which == 0 else (offset, 0)), flip_core)

    def flipped(bit, flip):
        return 1 - bit if flip else bit

    def pos_at(cls, offset):
        bits = (u, v)[cls]
        return (
            number([flipped(b, offset & (8 >> n)) for n, b in enumerate(bits)]) * 2
            + flipped(core, offset & 1)
        )

    def pair_at(cls, offset):
        bits = group[cls]
        return flipped(bits[0], offset & 2) * 2 + flipped(bits[1], offset & 1)

    barrier = pltpu.get_barrier_semaphore()

    def wait_bytes(view, sem):
        pltpu.make_async_copy(view, view, sem).wait()

    def tab_copy(block):
        cls, offset = block % 2, 3 - block // 2
        return pltpu.make_async_copy(
            tab_hbm.at[cls * 4 + pair_at(cls, offset)],
            tab.at[block],
            tab_sem.at[0 if block < 2 else 1],
        )

    def proof_copy(c, part_of):
        return pltpu.make_async_copy(proof_hbm.at[c], proof.at[c], proof_sem.at[part_of])

    for block in range(2):
        tab_copy(block).start()
    loads = ((0, 4), (4, 8), (8, CHANNELS))
    for part_of, (begin, end) in enumerate(loads):
        for c in range(begin, end):
            proof_copy(c, part_of).start()
    for block in range(2, 8):
        tab_copy(block).start()
    small = [
        pltpu.make_async_copy(target_hbm, target, small_sem.at[0]),
        pltpu.make_async_copy(ttab_hbm, ttab, small_sem.at[1]),
        pltpu.make_async_copy(loading_hbm, loading, small_sem.at[2]),
    ]
    for copy in small:
        copy.start()

    for other in OTHERS:
        for cls in range(2):
            pl.semaphore_signal(
                barrier, inc=1, device_id=place(cls, other // 2, other % 2), device_id_type=MESH
            )
    wait_bytes(tab.at[pl.ds(0, 2)], tab_sem.at[0])

    def spectra(begin, end, channels):
        lines = tab[begin:end].reshape((end - begin) * 64, 512)
        for c in channels:
            got = nt(lines, proof[c])
            start = c * STRIDE + begin * 64
            stage[0, start : start + (end - begin) * 64, :] = got[:, :128]
            stage[1, start : start + (end - begin) * 64, :] = got[:, 128:]

    def turn(block):
        def one(n, carry):
            for i in range(4):
                row = block * 64 + n * 4 + i
                low = stage[0, pl.ds(row, CHANNELS, stride=STRIDE), :]
                high = stage[1, pl.ds(row, CHANNELS, stride=STRIDE), :]
                xsend[row, :, 0:128] = low.astype(jnp.bfloat16)
                xsend[row, :, 128:256] = high.astype(jnp.bfloat16)
            return carry

        lax.fori_loop(0, POSITIONS, one, 0, unroll=4)

    def send_pair(offset, classes=(0, 1)):
        slot = 3 - offset
        base = [(slot * 2 + cls) * 64 for cls in range(2)]
        for other in OTHERS:
            for cls in classes:
                pltpu.make_async_remote_copy(
                    src_ref=xsend.at[pl.ds(base[cls] + pos_at(cls, other) * 4, 4)],
                    dst_ref=xrecv.at[cls, slot, :, mine[cls]],
                    send_sem=x_send_sem,
                    recv_sem=x_recv_sem.at[cls, slot],
                    device_id=place(cls, other // 2, other % 2),
                    device_id_type=MESH,
                ).start()
        for cls in classes:
            for i in range(4):
                xrecv[cls, slot, i, mine[cls]] = xsend[base[cls] + mine[cls] * 4 + i]

    def send_single(offset, classes=(0, 1)):
        slot = 3 - offset
        base = [
            ((3 - offset // 2) * 2 + cls) * 64 + flipped(group[cls][2], offset % 2) * 2
            for cls in range(2)
        ]
        for other in OTHERS:
            for cls in classes:
                pltpu.make_async_remote_copy(
                    src_ref=xsend.at[pl.ds(base[cls] + pos_at(cls, other) * 4, 2)],
                    dst_ref=xlast.at[cls, slot, :, mine[cls]],
                    send_sem=x_send_sem,
                    recv_sem=x_recv_sem.at[cls, 2 + slot],
                    device_id=place(cls, other // 2, other % 2),
                    device_id_type=MESH,
                ).start()
        for cls in classes:
            for i in range(2):
                xlast[cls, slot, i, mine[cls]] = xsend[base[cls] + mine[cls] * 4 + i]

    def along_positions(src, dst, sems):
        for other in OTHERS:
            pltpu.make_async_remote_copy(
                src_ref=src(pos_at(0, other)),
                dst_ref=dst(mine[0]),
                send_sem=sems.at[0],
                recv_sem=sems.at[1],
                device_id=place(0, other // 2, other % 2),
                device_id_type=MESH,
            ).start()

    def along_groups(src, dst, sems):
        here = number(v)
        for offset in range(1, GROUPS):
            there = number([flipped(bit, offset & (4 >> n)) for n, bit in enumerate(v)])
            pltpu.make_async_remote_copy(
                src_ref=src.at[there],
                dst_ref=dst.at[here],
                send_sem=sems.at[0],
                recv_sem=sems.at[1],
                device_id=place(1, offset),
                device_id_type=MESH,
            ).start()
        dst[here] = src[here]

    for part_of, (begin, end) in enumerate(loads):
        wait_bytes(proof.at[pl.ds(begin, end - begin)], proof_sem.at[part_of])
        spectra(0, 2, range(begin, end))
    turn(0)
    pl.semaphore_wait(barrier, 2 * len(OTHERS))
    send_pair(3, (0,))
    turn(1)
    send_pair(3, (1,))
    wait_bytes(tab.at[pl.ds(2, 6)], tab_sem.at[1])
    spectra(2, 8, range(CHANNELS))
    turn(2)
    turn(3)
    send_pair(2)
    turn(4)
    turn(5)
    for copy in small:
        copy.wait()
    rows[...] = nt(ttab[...], target[...])

    for pos in range(POSITIONS):
        for grp in range(GROUPS):
            at = (pos * GROUPS + grp) * 4
            tsend[pos, grp] = rows[at : at + 4, :].astype(jnp.bfloat16)
    along_positions(lambda p: tsend.at[p], lambda p: tpass.at[:, p], t_sem.at[0])
    for grp in range(GROUPS):
        tpass[grp, mine[0]] = tsend[mine[0], grp]

    send_single(3)
    turn(6)
    turn(7)

    def gram(re, im):
        re, im = re.reshape(256, 256), im.reshape(256, 256)
        ret, imt = re.T, im.T
        return (nn(ret, re) + nn(imt, im) + (nn(ret, im) - nn(imt, re))) * (1.0 / 256.0)

    def pair_grams(cls, offset):
        slot = 3 - offset
        wait_bytes(xrecv.at[cls, slot, :, pl.ds(0, POSITIONS - 1)], x_recv_sem.at[cls, slot])
        for bit in (1, 0):
            row = flipped(group[cls][2], bit) * 2
            part[cls, offset * 2 + bit] = gram(
                xrecv[cls, slot, row], xrecv[cls, slot, row + 1]
            )

    def single_gram(cls, offset):
        slot = 3 - offset
        wait_bytes(xlast.at[cls, slot, :, pl.ds(0, POSITIONS - 1)], x_recv_sem.at[cls, 2 + slot])
        part[cls, offset] = gram(xlast[cls, slot, 0], xlast[cls, slot, 1])

    def sem_of(cls, offset, piece):
        if offset == 0:
            return m_recv_sem.at[0]
        fed = [other for other in range(1, GROUPS) if feeders(other, piece)]
        return m_recv_sem.at[1 + (cls * 2 + piece) * 3 + fed.index(offset)]

    def wait_fed(cls, offset, piece):
        count = len(feeders(offset, piece))
        if count:
            wait_bytes(mrecv.at[cls, piece, pl.ds(0, count)], sem_of(cls, offset, piece))

    def wait_sums():
        wait_bytes(msend.at[pl.ds(0, 12)], sem_of(0, 0, 0))

    def gram_sum(cls, offset, piece):
        total = part[cls, offset, pl.ds(piece * PIECE, PIECE), :]
        for other in feeders(offset, piece):
            total = total + mrecv[cls, piece, other].astype(jnp.float32)
        return total

    def pass_on(cls, offset, piece):
        wait_fed(cls, offset, piece)
        at = cls * 16 + piece * GROUPS + offset
        msend[at] = gram_sum(cls, offset, piece).astype(jnp.bfloat16)
        pltpu.make_async_remote_copy(
            src_ref=msend.at[at],
            dst_ref=mrecv.at[cls, piece, offset],
            send_sem=m_send_sem,
            recv_sem=sem_of(cls, offset ^ next_bit(offset, piece), piece),
            device_id=place(1 - cls, next_bit(offset, piece)),
            device_id_type=MESH,
        ).start()

    for cls in range(2):
        pair_grams(cls, 3)
        pass_on(cls, 7, 1)
        pass_on(cls, 7, 0)
        pass_on(cls, 6, 0)
    send_single(2)
    for cls in range(2):
        pair_grams(cls, 2)
        pass_on(cls, 5, 1)
    send_single(1)
    wait_bytes(tpass.at[:, pl.ds(0, POSITIONS - 1)], t_sem.at[0, 1])
    along_groups(tpass, trecv, t_sem.at[1])
    for cls in range(2):
        pass_on(cls, 6, 1)
    for cls in range(2):
        pass_on(cls, 5, 0)
        pass_on(cls, 4, 0)
    for cls in range(2):
        single_gram(cls, 3)
        single_gram(cls, 2)
        pass_on(cls, 3, 1)
        pass_on(cls, 3, 0)
        pass_on(cls, 2, 0)
    send_single(0)
    for cls in range(2):
        pass_on(cls, 4, 1)
    for cls in range(2):
        single_gram(cls, 1)
        pass_on(cls, 1, 1)
        pass_on(cls, 1, 0)
    for cls in range(2):
        pass_on(cls, 2, 1)

    lane = lax.broadcasted_iota(jnp.int32, (16, 128), 1) // 32
    wait_bytes(trecv.at[pl.ds(0, GROUPS - 1)], t_sem.at[1, 1])
    for device in range(128):
        bits_v, bits_u, its_core = split_place(device // 8, device % 8)
        rows[device * 4 : device * 4 + 4, :] = trecv[
            number(bits_v), number(bits_u) * 2 + its_core
        ].astype(jnp.float32)
    for i in range(4):
        blocks = [rows[pl.ds(g * 4 + i, 16, stride=32), :] for g in range(8)]
        for t in range(4):
            for tile in range(2):
                total = jnp.zeros((16, 128), jnp.float32)
                for k in range(4):
                    turned = blocks[tile * 4 + k]
                    if k != t:
                        turned = pltpu.roll(turned, (32 * (k - t)) % 128, 1)
                    total = jnp.where(lane == k, turned, total)
                tmat[
                    i // 2, (i % 2) * 64 + t * 16 : (i % 2) * 64 + t * 16 + 16,
                    tile * 128 : tile * 128 + 128,
                ] = total.astype(jnp.bfloat16)

    for cls in range(2):
        single_gram(cls, 0)

    bins = bins_of(v, u, core)

    def combine(straight, turned):
        return (
            0.5 * (straight[:64] - straight[64:] + turned[:64] + turned[64:]),
            0.5 * (straight[:64] + straight[64:] - turned[:64] + turned[64:]),
        )

    def halves(whole):
        high = whole.astype(jnp.bfloat16)
        return high, (whole - high.astype(jnp.float32)).astype(jnp.bfloat16)

    wait_sums()
    both_grams = [
        halves(jnp.concatenate([gram_sum(cls, 0, piece) for piece in range(2)], axis=0))
        for cls in range(2)
    ]
    both_once = []
    for cls in range(2):
        (high, low), left = both_grams[cls], tmat[cls]
        both_once.append(
            combine(nn(left, high) + nn(left, low), nt(left, high) + nt(left, low))
        )
    both_twice = []
    for cls in range(2):
        high, low = both_grams[cls]
        once_high, once_low = halves(jnp.concatenate(both_once[cls], axis=0))
        lines = jnp.concatenate([once_high, once_low], axis=0)
        straight, turned = nn(lines, high), nt(lines, high)
        both_twice.append(
            combine(
                straight[:128] + straight[128:] + nn(once_high, low),
                turned[:128] + turned[128:] + nt(once_high, low),
            )
        )
    for cls in range(2):
        load = loading[bins[cls]]
        step = 1.0 / (load + rho)
        keep, take = 2.0 * step - load * step * step, step * step
        for side in range(2):
            pred = keep * both_once[cls][side] - take * both_twice[cls][side]
            for g in range(8):
                k, tile = g % 4, g // 4
                moved = jnp.zeros((16, 128), jnp.float32)
                for t in range(4):
                    turned = pred[t * 16 : t * 16 + 16, tile * 128 : tile * 128 + 128]
                    if k != t:
                        turned = pltpu.roll(turned, (32 * (t - k)) % 128, 1)
                    moved = jnp.where(lane == t, turned, moved)
                rows[pl.ds(g * 4 + cls * 2 + side, 16, stride=32), :] = moved

    me = gx * 8 + gy
    for device in range(128):
        psend[device] = rows[device * 4 : device * 4 + 4, :].astype(jnp.bfloat16)
    for by_v, by_u, flip_core in FAR_FIRST:
        row, column = place_off(by_v, by_u, flip_core)
        pltpu.make_async_remote_copy(
            src_ref=psend.at[row * 8 + column],
            dst_ref=precv.at[me],
            send_sem=p_sem.at[0],
            recv_sem=p_sem.at[1],
            device_id=(row, column),
            device_id_type=MESH,
        ).start()
    precv[me] = psend[me]
    wait_bytes(precv.at[pl.ds(0, 127)], p_sem.at[1])
    for device in range(128):
        rows[device * 4 : device * 4 + 4, :] = precv[device].astype(jnp.float32)
    out[...] = rows[...].astype(jnp.bfloat16)

    wait_bytes(xsend.at[pl.ds(0, 32 * (POSITIONS - 1))], x_send_sem)
    wait_bytes(msend.at[pl.ds(0, 4 * (GROUPS - 1))], m_send_sem)
    wait_bytes(tpass.at[:, pl.ds(0, POSITIONS - 1)], t_sem.at[0, 0])
    wait_bytes(trecv.at[pl.ds(0, GROUPS - 1)], t_sem.at[1, 0])
    wait_bytes(precv.at[pl.ds(0, 127)], p_sem.at[0])


def tables(length):
    forward, inverse = transform_tables(length)
    by_pair = (
        forward.reshape(2, POSITIONS, 4, 4, length)
        .transpose(0, 2, 1, 3, 4)
        .reshape(8, POSITIONS * 4, length)
    )
    first = []
    bits = [(n // 4, n // 2 % 2, n % 2) for n in range(GROUPS)]
    for pos in range(POSITIONS):
        for grp in range(GROUPS):
            for found in bins_of(bits[grp], bits[pos // 2], pos % 2):
                first += [2 * found, 2 * found + 1]
    second = []
    for device in range(128):
        for found in bins_of(*split_place(device // 8, device % 8)):
            second += [2 * found, 2 * found + 1]
    return tuple(
        jnp.asarray(table).astype(jnp.bfloat16)
        for table in (by_pair, forward[first], inverse[second])
    )


def local(proof, target, loading):
    channels, segments, length = proof.shape
    rho = (1.0 + math.sqrt(2048 / segments)) ** 2
    by_pair, by_owner, inverse = tables(length)
    bf16, f32 = jnp.bfloat16, jnp.float32
    hbm = pl.BlockSpec(memory_space=pltpu.HBM)
    scratch = [
        pltpu.VMEM((8, 64, 512), bf16),
        pltpu.VMEM((512, 512), bf16),
        pltpu.VMEM((16, 256, 512), bf16),
        pltpu.VMEM((128, 512), bf16),
        pltpu.SMEM((256,), f32),
        pltpu.VMEM((2, CHANNELS * STRIDE, 128), f32),
        pltpu.VMEM((512, CHANNELS, 256), bf16),
        pltpu.VMEM((2, 2, 4, POSITIONS, CHANNELS, 256), bf16),
        pltpu.VMEM((2, 4, 2, POSITIONS, CHANNELS, 256), bf16),
        pltpu.VMEM((2, GROUPS, 256, 256), f32),
        pltpu.VMEM((4 * GROUPS, PIECE, 256), bf16),
        pltpu.VMEM((2, 2, GROUPS, PIECE, 256), bf16),
        pltpu.VMEM((2, 128, 256), bf16),
        pltpu.VMEM((POSITIONS, GROUPS, 4, 128), bf16),
        pltpu.VMEM((GROUPS, POSITIONS, 4, 128), bf16),
        pltpu.VMEM((GROUPS, POSITIONS, 4, 128), bf16),
        pltpu.VMEM((512, 128), f32),
        pltpu.VMEM((128, 4, 128), bf16),
        pltpu.VMEM((128, 4, 128), bf16),
        pltpu.SemaphoreType.DMA((3,)),
        pltpu.SemaphoreType.DMA((2,)),
        pltpu.SemaphoreType.DMA((3,)),
        pltpu.SemaphoreType.DMA,
        pltpu.SemaphoreType.DMA((2, 6)),
        pltpu.SemaphoreType.DMA,
        pltpu.SemaphoreType.DMA((13,)),
        pltpu.SemaphoreType.DMA((2, 2)),
        pltpu.SemaphoreType.DMA((2,)),
    ]
    hold = [
        pltpu.with_memory_space_constraint(array, pltpu.HBM)
        for array in (by_pair, by_owner, proof, target.reshape(128, length), loading)
    ]
    spectra = pl.pallas_call(
        functools.partial(kernel, rho),
        out_shape=jax.ShapeDtypeStruct((512, 128), bf16),
        in_specs=[hbm] * 5,
        out_specs=pl.BlockSpec(memory_space=pltpu.VMEM),
        scratch_shapes=scratch,
        compiler_params=pltpu.CompilerParams(
            collective_id=0, has_side_effects=True, vmem_limit_bytes=40 * 2**20
        ),
    )(*hold)
    return tn(spectra, inverse).reshape(4, 32, length)


def solution(mesh):
    return jax.shard_map(
        local,
        mesh=mesh,
        in_specs=(P(("gx", "gy"), None, None), P("gx", "gy", None), P()),
        out_specs=P("gx", "gy", None),
        check_vma=False,
    )
```

```python
import functools
import math

import jax
import jax.numpy as jnp
import numpy as np
from jax import lax
from jax.experimental import pallas as pl
from jax.experimental.pallas import tpu as pltpu
from jax.sharding import PartitionSpec as P

GROUPS = 8
POSITIONS = 16
CHANNELS = 16
STRIDE = 520
OTHERS = (14, 12, 6, 10, 8, 4, 2, 15, 13, 7, 11, 9, 5, 3, 1)
FAR_FIRST = sorted(
    ((v, u, core) for v in range(8) for u in range(8) for core in range(2) if v or u or core),
    key=lambda way: -(way[0].bit_count() + way[1].bit_count()),
)
PIECE = 128
ORDERS = ((2, 4, 1), (1, 4, 2))
MESH = pl.DeviceIdType.MESH


def transform_tables(length):
    half = length // 2
    sample = np.arange(length)
    phase = ((np.arange(half)[:, None] * sample[None, :]) % length).astype(np.float32) * np.float32(
        2.0 * math.pi / length
    )
    angle = sample.astype(np.float32) * np.float32(2.0 * math.pi / length)
    window = np.float32(0.5) - np.float32(0.5) * np.cos(angle)
    forward = np.stack([window * np.cos(phase), -window * np.sin(phase)], axis=1).reshape(
        length, length
    ) * np.float32(1.0 / math.sqrt(0.375 * length))
    inverse = np.stack([np.cos(phase), -np.sin(phase)], axis=1).reshape(
        length, length
    ) * np.float32(math.sqrt(2.0 / length))
    return forward.astype(np.float32), inverse.astype(np.float32)


def split_place(gx, gy):
    core, z, yh = gx % 2, (gx // 2) % 4, gx // 8
    x, yl = gy % 4, gy // 4
    v = (z // 2, yh, x // 2)
    return v, ((z + v[0]) % 2, (yl + yh) % 2, (x + v[2]) % 2), core


def number(bits):
    return (bits[0] * 2 + bits[1]) * 2 + bits[2]


def bins_of(v, u, core):
    return (
        (number(u) * 2 + core) * GROUPS + number(v),
        128 + (number(v) * 2 + core) * GROUPS + number(u),
    )


def next_bit(offset, piece):
    return next(bit for bit in ORDERS[piece] if offset & bit)


def feeders(offset, piece):
    return [
        other for other in range(1, GROUPS) if other ^ next_bit(other, piece) == offset
    ]


def nt(left, right):
    return lax.dot_general(
        left, right, (((1,), (1,)), ((), ())), preferred_element_type=jnp.float32
    )


def nn(left, right):
    return lax.dot_general(
        left, right, (((1,), (0,)), ((), ())), preferred_element_type=jnp.float32
    )


def tn(left, right):
    return lax.dot_general(
        left, right, (((0,), (0,)), ((), ())), preferred_element_type=jnp.float32
    )


def kernel(
    rho,
    tab_hbm, ttab_hbm, proof_hbm, target_hbm, loading_hbm,
    out,
    tab, ttab, proof, target, loading,
    stage, xsend, xrecv, xlast, part, msend, mrecv, tmat, tsend, tpass, trecv, rows, psend, precv,
    proof_sem, tab_sem, small_sem,
    x_send_sem, x_recv_sem, m_send_sem, m_recv_sem, t_sem, p_sem,
):
    gx, gy = lax.axis_index("gx"), lax.axis_index("gy")
    v, u, core = split_place(gx, gy)
    group = (v, u)
    mine = (number(u) * 2 + core, number(v) * 2 + core)

    z, yh, x, yl = (gx // 2) % 4, gx // 8, gy % 4, gy // 4
    z_flip = (2 * v[0] + 1 - z % 2, 2 * (1 - v[0]) + 1 - z % 2, 2 * (1 - v[0]) + z % 2)
    x_flip = (2 * v[2] + 1 - x % 2, 2 * (1 - v[2]) + 1 - x % 2, 2 * (1 - v[2]) + x % 2)

    def place_off(by_v, by_u, flip_core=0):
        turns_z = (z, z_flip[0], z_flip[1], z_flip[2])
        turns_x = (x, x_flip[0], x_flip[1], x_flip[2])
        there_z = turns_z[(by_v >> 2 & 1) * 2 + (by_u >> 2 & 1)]
        there_x = turns_x[(by_v & 1) * 2 + (by_u & 1)]
        there_yh = 1 - yh if by_v & 2 else yh
        there_yl = 1 - yl if (by_v ^ by_u) & 2 else yl
        there_core = 1 - core if flip_core else core
        return there_yh * 8 + there_z * 2 + there_core, there_yl * 4 + there_x

    def place(which, offset, flip_core=0):
        return place_off(*((0, offset) if which == 0 else (offset, 0)), flip_core)

    def flipped(bit, flip):
        return 1 - bit if flip else bit

    def pos_at(cls, offset):
        bits = (u, v)[cls]
        return (
            number([flipped(b, offset & (8 >> n)) for n, b in enumerate(bits)]) * 2
            + flipped(core, offset & 1)
        )

    def pair_at(cls, offset):
        bits = group[cls]
        return flipped(bits[0], offset & 2) * 2 + flipped(bits[1], offset & 1)

    barrier = pltpu.get_barrier_semaphore()

    def wait_bytes(view, sem):
        pltpu.make_async_copy(view, view, sem).wait()

    def tab_copy(block):
        cls, offset = block % 2, 3 - block // 2
        return pltpu.make_async_copy(
            tab_hbm.at[cls * 4 + pair_at(cls, offset)],
            tab.at[block],
            tab_sem.at[0 if block < 2 else 1],
        )

    def proof_copy(c, part_of):
        return pltpu.make_async_copy(proof_hbm.at[c], proof.at[c], proof_sem.at[part_of])

    for block in range(2):
        tab_copy(block).start()
    loads = ((0, 6), (6, CHANNELS))
    for part_of, (begin, end) in enumerate(loads):
        for c in range(begin, end):
            proof_copy(c, part_of).start()
    for block in range(2, 8):
        tab_copy(block).start()
    small = [
        pltpu.make_async_copy(target_hbm, target, small_sem.at[0]),
        pltpu.make_async_copy(ttab_hbm, ttab, small_sem.at[1]),
        pltpu.make_async_copy(loading_hbm, loading, small_sem.at[2]),
    ]
    for copy in small:
        copy.start()

    for other in OTHERS:
        for cls in range(2):
            pl.semaphore_signal(
                barrier, inc=1, device_id=place(cls, other // 2, other % 2), device_id_type=MESH
            )
    wait_bytes(tab.at[pl.ds(0, 2)], tab_sem.at[0])

    def spectra(begin, end, channels):
        lines = tab[begin:end].reshape((end - begin) * 64, 512)
        for c in channels:
            got = nt(lines, proof[c])
            start = c * STRIDE + begin * 64
            stage[0, start : start + (end - begin) * 64, :] = got[:, :128]
            stage[1, start : start + (end - begin) * 64, :] = got[:, 128:]

    def turn(block):
        def one(n, carry):
            for i in range(4):
                row = block * 64 + n * 4 + i
                low = stage[0, pl.ds(row, CHANNELS, stride=STRIDE), :]
                high = stage[1, pl.ds(row, CHANNELS, stride=STRIDE), :]
                xsend[row, :, 0:128] = low.astype(jnp.bfloat16)
                xsend[row, :, 128:256] = high.astype(jnp.bfloat16)
            return carry

        lax.fori_loop(0, POSITIONS, one, 0, unroll=4)

    def send_pair(offset, classes=(0, 1)):
        slot = 3 - offset
        base = [(slot * 2 + cls) * 64 for cls in range(2)]
        for other in OTHERS:
            for cls in classes:
                pltpu.make_async_remote_copy(
                    src_ref=xsend.at[pl.ds(base[cls] + pos_at(cls, other) * 4, 4)],
                    dst_ref=xrecv.at[cls, slot, :, mine[cls]],
                    send_sem=x_send_sem,
                    recv_sem=x_recv_sem.at[cls, slot],
                    device_id=place(cls, other // 2, other % 2),
                    device_id_type=MESH,
                ).start()
        for cls in classes:
            for i in range(4):
                xrecv[cls, slot, i, mine[cls]] = xsend[base[cls] + mine[cls] * 4 + i]

    def send_single(offset, classes=(0, 1)):
        slot = 3 - offset
        base = [
            ((3 - offset // 2) * 2 + cls) * 64 + flipped(group[cls][2], offset % 2) * 2
            for cls in range(2)
        ]
        for other in OTHERS:
            for cls in classes:
                pltpu.make_async_remote_copy(
                    src_ref=xsend.at[pl.ds(base[cls] + pos_at(cls, other) * 4, 2)],
                    dst_ref=xlast.at[cls, slot, :, mine[cls]],
                    send_sem=x_send_sem,
                    recv_sem=x_recv_sem.at[cls, 2 + slot],
                    device_id=place(cls, other // 2, other % 2),
                    device_id_type=MESH,
                ).start()
        for cls in classes:
            for i in range(2):
                xlast[cls, slot, i, mine[cls]] = xsend[base[cls] + mine[cls] * 4 + i]

    def along_positions(src, dst, sems):
        for other in OTHERS:
            pltpu.make_async_remote_copy(
                src_ref=src(pos_at(0, other)),
                dst_ref=dst(mine[0]),
                send_sem=sems.at[0],
                recv_sem=sems.at[1],
                device_id=place(0, other // 2, other % 2),
                device_id_type=MESH,
            ).start()

    def along_groups(src, dst, sems):
        here = number(v)
        for offset in range(1, GROUPS):
            there = number([flipped(bit, offset & (4 >> n)) for n, bit in enumerate(v)])
            pltpu.make_async_remote_copy(
                src_ref=src.at[there],
                dst_ref=dst.at[here],
                send_sem=sems.at[0],
                recv_sem=sems.at[1],
                device_id=place(1, offset),
                device_id_type=MESH,
            ).start()
        dst[here] = src[here]

    for part_of, (begin, end) in enumerate(loads):
        wait_bytes(proof.at[pl.ds(begin, end - begin)], proof_sem.at[part_of])
        spectra(0, 2, range(begin, end))
    turn(0)
    pl.semaphore_wait(barrier, 2 * len(OTHERS))
    send_pair(3, (0,))
    turn(1)
    send_pair(3, (1,))
    wait_bytes(tab.at[pl.ds(2, 6)], tab_sem.at[1])
    spectra(2, 8, range(CHANNELS))
    turn(2)
    turn(3)
    send_pair(2)
    turn(4)
    turn(5)
    for copy in small:
        copy.wait()
    rows[...] = nt(ttab[...], target[...])

    for pos in range(POSITIONS):
        for grp in range(GROUPS):
            at = (pos * GROUPS + grp) * 4
            tsend[pos, grp] = rows[at : at + 4, :].astype(jnp.bfloat16)
    along_positions(lambda p: tsend.at[p], lambda p: tpass.at[:, p], t_sem.at[0])
    for grp in range(GROUPS):
        tpass[grp, mine[0]] = tsend[mine[0], grp]

    send_single(3)
    turn(6)
    turn(7)

    def gram(re, im):
        re, im = re.reshape(256, 256), im.reshape(256, 256)
        ret, imt = re.T, im.T
        return (nn(ret, re) + nn(imt, im) + (nn(ret, im) - nn(imt, re))) * (1.0 / 256.0)

    def pair_grams(cls, offset):
        slot = 3 - offset
        wait_bytes(xrecv.at[cls, slot, :, pl.ds(0, POSITIONS - 1)], x_recv_sem.at[cls, slot])
        for bit in (1, 0):
            row = flipped(group[cls][2], bit) * 2
            part[cls, offset * 2 + bit] = gram(
                xrecv[cls, slot, row], xrecv[cls, slot, row + 1]
            )

    def wait_single(cls, offset):
        slot = 3 - offset
        wait_bytes(xlast.at[cls, slot, :, pl.ds(0, POSITIONS - 1)], x_recv_sem.at[cls, 2 + slot])

    def arrived_gram(cls, offset):
        slot = 3 - offset
        part[cls, offset] = gram(xlast[cls, slot, 0], xlast[cls, slot, 1])

    def single_gram(cls, offset):
        wait_single(cls, offset)
        arrived_gram(cls, offset)

    def sem_of(cls, offset, piece):
        if offset == 0:
            return m_recv_sem.at[0]
        fed = [other for other in range(1, GROUPS) if feeders(other, piece)]
        return m_recv_sem.at[1 + (cls * 2 + piece) * 3 + fed.index(offset)]

    def wait_fed(cls, offset, piece):
        count = len(feeders(offset, piece))
        if count:
            wait_bytes(mrecv.at[cls, piece, pl.ds(0, count)], sem_of(cls, offset, piece))

    def wait_sums():
        wait_bytes(msend.at[pl.ds(0, 12)], sem_of(0, 0, 0))

    def gram_sum(cls, offset, piece):
        total = part[cls, offset, pl.ds(piece * PIECE, PIECE), :]
        for other in feeders(offset, piece):
            total = total + mrecv[cls, piece, other].astype(jnp.float32)
        return total

    def pass_on(cls, offset, piece):
        wait_fed(cls, offset, piece)
        at = cls * 16 + piece * GROUPS + offset
        msend[at] = gram_sum(cls, offset, piece).astype(jnp.bfloat16)
        pltpu.make_async_remote_copy(
            src_ref=msend.at[at],
            dst_ref=mrecv.at[cls, piece, offset],
            send_sem=m_send_sem,
            recv_sem=sem_of(cls, offset ^ next_bit(offset, piece), piece),
            device_id=place(1 - cls, next_bit(offset, piece)),
            device_id_type=MESH,
        ).start()

    for cls in range(2):
        pair_grams(cls, 3)
        pass_on(cls, 7, 1)
        pass_on(cls, 7, 0)
        pass_on(cls, 6, 0)
    send_single(2)
    for cls in range(2):
        pair_grams(cls, 2)
        pass_on(cls, 5, 1)
    send_single(1)
    wait_bytes(tpass.at[:, pl.ds(0, POSITIONS - 1)], t_sem.at[0, 1])
    along_groups(tpass, trecv, t_sem.at[1])
    for cls in range(2):
        pass_on(cls, 6, 1)
    for cls in range(2):
        pass_on(cls, 5, 0)
        pass_on(cls, 4, 0)
    for cls in range(2):
        single_gram(cls, 3)
        single_gram(cls, 2)
        pass_on(cls, 3, 1)
        pass_on(cls, 3, 0)
        pass_on(cls, 2, 0)
    send_single(0)
    for cls in range(2):
        pass_on(cls, 4, 1)
    for cls in range(2):
        single_gram(cls, 1)
        pass_on(cls, 1, 1)
        pass_on(cls, 1, 0)
    for cls in range(2):
        pass_on(cls, 2, 1)

    lane = lax.broadcasted_iota(jnp.int32, (16, 128), 1) // 32
    wait_bytes(trecv.at[pl.ds(0, GROUPS - 1)], t_sem.at[1, 1])
    for device in range(128):
        bits_v, bits_u, its_core = split_place(device // 8, device % 8)
        rows[device * 4 : device * 4 + 4, :] = trecv[
            number(bits_v), number(bits_u) * 2 + its_core
        ].astype(jnp.float32)
    for i in range(4):
        blocks = [rows[pl.ds(g * 4 + i, 16, stride=32), :] for g in range(8)]
        for t in range(4):
            for tile in range(2):
                total = jnp.zeros((16, 128), jnp.float32)
                for k in range(4):
                    turned = blocks[tile * 4 + k]
                    if k != t:
                        turned = pltpu.roll(turned, (32 * (k - t)) % 128, 1)
                    total = jnp.where(lane == k, turned, total)
                tmat[
                    i // 2, (i % 2) * 64 + t * 16 : (i % 2) * 64 + t * 16 + 16,
                    tile * 128 : tile * 128 + 128,
                ] = total.astype(jnp.bfloat16)

    for cls in range(2):
        wait_single(cls, 0)
    for cls in range(2):
        arrived_gram(cls, 0)

    bins = bins_of(v, u, core)

    def combine(straight, turned):
        return (
            0.5 * (straight[:64] - straight[64:] + turned[:64] + turned[64:]),
            0.5 * (straight[:64] + straight[64:] - turned[:64] + turned[64:]),
        )

    def halves(whole):
        high = whole.astype(jnp.bfloat16)
        return high, (whole - high.astype(jnp.float32)).astype(jnp.bfloat16)

    wait_sums()
    both_grams = [
        halves(jnp.concatenate([gram_sum(cls, 0, piece) for piece in range(2)], axis=0))
        for cls in range(2)
    ]
    both_once = []
    for cls in range(2):
        (high, low), left = both_grams[cls], tmat[cls]
        both_once.append(
            combine(nn(left, high) + nn(left, low), nt(left, high) + nt(left, low))
        )
    both_twice = []
    for cls in range(2):
        high, low = both_grams[cls]
        once_high, once_low = halves(jnp.concatenate(both_once[cls], axis=0))
        lines = jnp.concatenate([once_high, once_low], axis=0)
        straight, turned = nn(lines, high), nt(lines, high)
        both_twice.append(
            combine(
                straight[:128] + straight[128:] + nn(once_high, low),
                turned[:128] + turned[128:] + nt(once_high, low),
            )
        )
    for cls in range(2):
        load = loading[bins[cls]]
        step = 1.0 / (load + rho)
        keep, take = 2.0 * step - load * step * step, step * step
        for side in range(2):
            pred = keep * both_once[cls][side] - take * both_twice[cls][side]
            for g in range(8):
                k, tile = g % 4, g // 4
                moved = jnp.zeros((16, 128), jnp.float32)
                for t in range(4):
                    turned = pred[t * 16 : t * 16 + 16, tile * 128 : tile * 128 + 128]
                    if k != t:
                        turned = pltpu.roll(turned, (32 * (t - k)) % 128, 1)
                    moved = jnp.where(lane == t, turned, moved)
                rows[pl.ds(g * 4 + cls * 2 + side, 16, stride=32), :] = moved

    me = gx * 8 + gy
    for device in range(128):
        psend[device] = rows[device * 4 : device * 4 + 4, :].astype(jnp.bfloat16)
    for by_v, by_u, flip_core in FAR_FIRST:
        row, column = place_off(by_v, by_u, flip_core)
        pltpu.make_async_remote_copy(
            src_ref=psend.at[row * 8 + column],
            dst_ref=precv.at[me],
            send_sem=p_sem.at[0],
            recv_sem=p_sem.at[1],
            device_id=(row, column),
            device_id_type=MESH,
        ).start()
    precv[me] = psend[me]
    wait_bytes(precv.at[pl.ds(0, 127)], p_sem.at[1])
    for device in range(128):
        rows[device * 4 : device * 4 + 4, :] = precv[device].astype(jnp.float32)
    out[...] = rows[...].astype(jnp.bfloat16)

    wait_bytes(xsend.at[pl.ds(0, 32 * (POSITIONS - 1))], x_send_sem)
    wait_bytes(msend.at[pl.ds(0, 4 * (GROUPS - 1))], m_send_sem)
    wait_bytes(tpass.at[:, pl.ds(0, POSITIONS - 1)], t_sem.at[0, 0])
    wait_bytes(trecv.at[pl.ds(0, GROUPS - 1)], t_sem.at[1, 0])
    wait_bytes(precv.at[pl.ds(0, 127)], p_sem.at[0])


def tables(length):
    forward, inverse = transform_tables(length)
    by_pair = (
        forward.reshape(2, POSITIONS, 4, 4, length)
        .transpose(0, 2, 1, 3, 4)
        .reshape(8, POSITIONS * 4, length)
    )
    first = []
    bits = [(n // 4, n // 2 % 2, n % 2) for n in range(GROUPS)]
    for pos in range(POSITIONS):
        for grp in range(GROUPS):
            for found in bins_of(bits[grp], bits[pos // 2], pos % 2):
                first += [2 * found, 2 * found + 1]
    second = []
    for device in range(128):
        for found in bins_of(*split_place(device // 8, device % 8)):
            second += [2 * found, 2 * found + 1]
    return tuple(
        jnp.asarray(table).astype(jnp.bfloat16)
        for table in (by_pair, forward[first], inverse[second])
    )


def local(proof, target, loading):
    channels, segments, length = proof.shape
    rho = (1.0 + math.sqrt(2048 / segments)) ** 2
    by_pair, by_owner, inverse = tables(length)
    bf16, f32 = jnp.bfloat16, jnp.float32
    hbm = pl.BlockSpec(memory_space=pltpu.HBM)
    scratch = [
        pltpu.VMEM((8, 64, 512), bf16),
        pltpu.VMEM((512, 512), bf16),
        pltpu.VMEM((16, 256, 512), bf16),
        pltpu.VMEM((128, 512), bf16),
        pltpu.SMEM((256,), f32),
        pltpu.VMEM((2, CHANNELS * STRIDE, 128), f32),
        pltpu.VMEM((512, CHANNELS, 256), bf16),
        pltpu.VMEM((2, 2, 4, POSITIONS, CHANNELS, 256), bf16),
        pltpu.VMEM((2, 4, 2, POSITIONS, CHANNELS, 256), bf16),
        pltpu.VMEM((2, GROUPS, 256, 256), f32),
        pltpu.VMEM((4 * GROUPS, PIECE, 256), bf16),
        pltpu.VMEM((2, 2, GROUPS, PIECE, 256), bf16),
        pltpu.VMEM((2, 128, 256), bf16),
        pltpu.VMEM((POSITIONS, GROUPS, 4, 128), bf16),
        pltpu.VMEM((GROUPS, POSITIONS, 4, 128), bf16),
        pltpu.VMEM((GROUPS, POSITIONS, 4, 128), bf16),
        pltpu.VMEM((512, 128), f32),
        pltpu.VMEM((128, 4, 128), bf16),
        pltpu.VMEM((128, 4, 128), bf16),
        pltpu.SemaphoreType.DMA((3,)),
        pltpu.SemaphoreType.DMA((2,)),
        pltpu.SemaphoreType.DMA((3,)),
        pltpu.SemaphoreType.DMA,
        pltpu.SemaphoreType.DMA((2, 6)),
        pltpu.SemaphoreType.DMA,
        pltpu.SemaphoreType.DMA((13,)),
        pltpu.SemaphoreType.DMA((2, 2)),
        pltpu.SemaphoreType.DMA((2,)),
    ]
    hold = [
        pltpu.with_memory_space_constraint(array, pltpu.HBM)
        for array in (by_pair, by_owner, proof, target.reshape(128, length), loading)
    ]
    spectra = pl.pallas_call(
        functools.partial(kernel, rho),
        out_shape=jax.ShapeDtypeStruct((512, 128), bf16),
        in_specs=[hbm] * 5,
        out_specs=pl.BlockSpec(memory_space=pltpu.VMEM),
        scratch_shapes=scratch,
        compiler_params=pltpu.CompilerParams(
            collective_id=0, has_side_effects=True, vmem_limit_bytes=40 * 2**20
        ),
    )(*hold)
    return tn(spectra, inverse).reshape(4, 32, length)


def solution(mesh):
    return jax.shard_map(
        local,
        mesh=mesh,
        in_specs=(P(("gx", "gy"), None, None), P("gx", "gy", None), P()),
        out_specs=P("gx", "gy", None),
        check_vma=False,
    )
```

```python
import functools
import math

import jax
import jax.numpy as jnp
import numpy as np
from jax import lax
from jax.experimental import pallas as pl
from jax.experimental.pallas import tpu as pltpu
from jax.sharding import PartitionSpec as P

GROUPS = 8
POSITIONS = 16
CHANNELS = 16
STRIDE = 520
OTHERS = (14, 12, 6, 10, 8, 4, 2, 15, 13, 7, 11, 9, 5, 3, 1)
FAR_FIRST = sorted(
    ((v, u, core) for v in range(8) for u in range(8) for core in range(2) if v or u or core),
    key=lambda way: -(way[0].bit_count() + way[1].bit_count()),
)
PIECE = 128
ORDERS = ((2, 4, 1), (1, 4, 2))
MESH = pl.DeviceIdType.MESH


def transform_tables(length):
    half = length // 2
    sample = np.arange(length)
    phase = ((np.arange(half)[:, None] * sample[None, :]) % length).astype(np.float32) * np.float32(
        2.0 * math.pi / length
    )
    angle = sample.astype(np.float32) * np.float32(2.0 * math.pi / length)
    window = np.float32(0.5) - np.float32(0.5) * np.cos(angle)
    forward = np.stack([window * np.cos(phase), -window * np.sin(phase)], axis=1).reshape(
        length, length
    ) * np.float32(1.0 / math.sqrt(0.375 * length))
    inverse = np.stack([np.cos(phase), -np.sin(phase)], axis=1).reshape(
        length, length
    ) * np.float32(math.sqrt(2.0 / length))
    return forward.astype(np.float32), inverse.astype(np.float32)


def split_place(gx, gy):
    core, z, yh = gx % 2, (gx // 2) % 4, gx // 8
    x, yl = gy % 4, gy // 4
    v = (z // 2, yh, x // 2)
    return v, ((z + v[0]) % 2, (yl + yh) % 2, (x + v[2]) % 2), core


def number(bits):
    return (bits[0] * 2 + bits[1]) * 2 + bits[2]


def bins_of(v, u, core):
    return (
        (number(u) * 2 + core) * GROUPS + number(v),
        128 + (number(v) * 2 + core) * GROUPS + number(u),
    )


def next_bit(offset, piece):
    return next(bit for bit in ORDERS[piece] if offset & bit)


def feeders(offset, piece):
    return [
        other for other in range(1, GROUPS) if other ^ next_bit(other, piece) == offset
    ]


def nt(left, right):
    return lax.dot_general(
        left, right, (((1,), (1,)), ((), ())), preferred_element_type=jnp.float32
    )


def nn(left, right):
    return lax.dot_general(
        left, right, (((1,), (0,)), ((), ())), preferred_element_type=jnp.float32
    )


def tn(left, right):
    return lax.dot_general(
        left, right, (((0,), (0,)), ((), ())), preferred_element_type=jnp.float32
    )


def kernel(
    rho,
    tab_hbm, ttab_hbm, proof_hbm, target_hbm, loading_hbm,
    out,
    tab, ttab, proof, target, loading,
    stage, xsend, xrecv, xlast, part, msend, mrecv, tmat, tsend, tpass, trecv, rows, psend, precv,
    proof_sem, tab_sem, small_sem,
    x_send_sem, x_recv_sem, m_send_sem, m_recv_sem, t_sem, p_sem,
):
    gx, gy = lax.axis_index("gx"), lax.axis_index("gy")
    v, u, core = split_place(gx, gy)
    group = (v, u)
    mine = (number(u) * 2 + core, number(v) * 2 + core)

    z, yh, x, yl = (gx // 2) % 4, gx // 8, gy % 4, gy // 4
    z_flip = (2 * v[0] + 1 - z % 2, 2 * (1 - v[0]) + 1 - z % 2, 2 * (1 - v[0]) + z % 2)
    x_flip = (2 * v[2] + 1 - x % 2, 2 * (1 - v[2]) + 1 - x % 2, 2 * (1 - v[2]) + x % 2)

    def place_off(by_v, by_u, flip_core=0):
        turns_z = (z, z_flip[0], z_flip[1], z_flip[2])
        turns_x = (x, x_flip[0], x_flip[1], x_flip[2])
        there_z = turns_z[(by_v >> 2 & 1) * 2 + (by_u >> 2 & 1)]
        there_x = turns_x[(by_v & 1) * 2 + (by_u & 1)]
        there_yh = 1 - yh if by_v & 2 else yh
        there_yl = 1 - yl if (by_v ^ by_u) & 2 else yl
        there_core = 1 - core if flip_core else core
        return there_yh * 8 + there_z * 2 + there_core, there_yl * 4 + there_x

    def place(which, offset, flip_core=0):
        return place_off(*((0, offset) if which == 0 else (offset, 0)), flip_core)

    def flipped(bit, flip):
        return 1 - bit if flip else bit

    def pos_at(cls, offset):
        bits = (u, v)[cls]
        return (
            number([flipped(b, offset & (8 >> n)) for n, b in enumerate(bits)]) * 2
            + flipped(core, offset & 1)
        )

    def pair_at(cls, offset):
        bits = group[cls]
        return flipped(bits[0], offset & 2) * 2 + flipped(bits[1], offset & 1)

    barrier = pltpu.get_barrier_semaphore()

    def wait_bytes(view, sem):
        pltpu.make_async_copy(view, view, sem).wait()

    def tab_copy(block):
        cls, offset = block % 2, 3 - block // 2
        return pltpu.make_async_copy(
            tab_hbm.at[cls * 4 + pair_at(cls, offset)],
            tab.at[block],
            tab_sem.at[0 if block < 2 else 1],
        )

    def proof_copy(c, part_of):
        return pltpu.make_async_copy(proof_hbm.at[c], proof.at[c], proof_sem.at[part_of])

    for block in range(2):
        tab_copy(block).start()
    loads = ((0, 6), (6, CHANNELS))
    for c in range(*loads[0]):
        proof_copy(c, 0).start()

    for other in OTHERS:
        for cls in range(2):
            pl.semaphore_signal(
                barrier, inc=1, device_id=place(cls, other // 2, other % 2), device_id_type=MESH
            )

    for c in range(*loads[1]):
        proof_copy(c, 1).start()
    for block in range(2, 8):
        tab_copy(block).start()
    small = [
        pltpu.make_async_copy(target_hbm, target, small_sem.at[0]),
        pltpu.make_async_copy(ttab_hbm, ttab, small_sem.at[1]),
        pltpu.make_async_copy(loading_hbm, loading, small_sem.at[2]),
    ]
    for copy in small:
        copy.start()

    wait_bytes(tab.at[pl.ds(0, 2)], tab_sem.at[0])

    def spectra(begin, end, channels):
        lines = tab[begin:end].reshape((end - begin) * 64, 512)
        for c in channels:
            got = nt(lines, proof[c])
            start = c * STRIDE + begin * 64
            stage[0, start : start + (end - begin) * 64, :] = got[:, :128]
            stage[1, start : start + (end - begin) * 64, :] = got[:, 128:]

    def turn(block):
        def one(n, carry):
            for i in range(4):
                row = block * 64 + n * 4 + i
                low = stage[0, pl.ds(row, CHANNELS, stride=STRIDE), :]
                high = stage[1, pl.ds(row, CHANNELS, stride=STRIDE), :]
                xsend[row, :, 0:128] = low.astype(jnp.bfloat16)
                xsend[row, :, 128:256] = high.astype(jnp.bfloat16)
            return carry

        lax.fori_loop(0, POSITIONS, one, 0, unroll=4)

    def send_pair(offset, classes=(0, 1)):
        slot = 3 - offset
        base = [(slot * 2 + cls) * 64 for cls in range(2)]
        for other in OTHERS:
            for cls in classes:
                pltpu.make_async_remote_copy(
                    src_ref=xsend.at[pl.ds(base[cls] + pos_at(cls, other) * 4, 4)],
                    dst_ref=xrecv.at[cls, slot, :, mine[cls]],
                    send_sem=x_send_sem,
                    recv_sem=x_recv_sem.at[cls, slot],
                    device_id=place(cls, other // 2, other % 2),
                    device_id_type=MESH,
                ).start()
        for cls in classes:
            for i in range(4):
                xrecv[cls, slot, i, mine[cls]] = xsend[base[cls] + mine[cls] * 4 + i]

    def send_single(offset, classes=(0, 1)):
        slot = 3 - offset
        base = [
            ((3 - offset // 2) * 2 + cls) * 64 + flipped(group[cls][2], offset % 2) * 2
            for cls in range(2)
        ]
        for other in OTHERS:
            for cls in classes:
                pltpu.make_async_remote_copy(
                    src_ref=xsend.at[pl.ds(base[cls] + pos_at(cls, other) * 4, 2)],
                    dst_ref=xlast.at[cls, slot, :, mine[cls]],
                    send_sem=x_send_sem,
                    recv_sem=x_recv_sem.at[cls, 2 + slot],
                    device_id=place(cls, other // 2, other % 2),
                    device_id_type=MESH,
                ).start()
        for cls in classes:
            for i in range(2):
                xlast[cls, slot, i, mine[cls]] = xsend[base[cls] + mine[cls] * 4 + i]

    def along_positions(src, dst, sems):
        for other in OTHERS:
            pltpu.make_async_remote_copy(
                src_ref=src(pos_at(0, other)),
                dst_ref=dst(mine[0]),
                send_sem=sems.at[0],
                recv_sem=sems.at[1],
                device_id=place(0, other // 2, other % 2),
                device_id_type=MESH,
            ).start()

    def along_groups(src, dst, sems):
        here = number(v)
        for offset in range(1, GROUPS):
            there = number([flipped(bit, offset & (4 >> n)) for n, bit in enumerate(v)])
            pltpu.make_async_remote_copy(
                src_ref=src.at[there],
                dst_ref=dst.at[here],
                send_sem=sems.at[0],
                recv_sem=sems.at[1],
                device_id=place(1, offset),
                device_id_type=MESH,
            ).start()
        dst[here] = src[here]

    for part_of, (begin, end) in enumerate(loads):
        wait_bytes(proof.at[pl.ds(begin, end - begin)], proof_sem.at[part_of])
        spectra(0, 2, range(begin, end))
    turn(0)
    pl.semaphore_wait(barrier, 2 * len(OTHERS))
    send_pair(3, (0,))
    turn(1)
    send_pair(3, (1,))
    wait_bytes(tab.at[pl.ds(2, 6)], tab_sem.at[1])
    spectra(2, 8, range(CHANNELS))
    turn(2)
    turn(3)
    send_pair(2)
    turn(4)
    turn(5)
    for copy in small:
        copy.wait()
    rows[...] = nt(ttab[...], target[...])

    for pos in range(POSITIONS):
        for grp in range(GROUPS):
            at = (pos * GROUPS + grp) * 4
            tsend[pos, grp] = rows[at : at + 4, :].astype(jnp.bfloat16)
    along_positions(lambda p: tsend.at[p], lambda p: tpass.at[:, p], t_sem.at[0])
    for grp in range(GROUPS):
        tpass[grp, mine[0]] = tsend[mine[0], grp]

    send_single(3)
    turn(6)
    turn(7)

    def gram(re, im):
        re, im = re.reshape(256, 256), im.reshape(256, 256)
        ret, imt = re.T, im.T
        return (nn(ret, re) + nn(imt, im) + (nn(ret, im) - nn(imt, re))) * (1.0 / 256.0)

    def pair_grams(cls, offset):
        slot = 3 - offset
        wait_bytes(xrecv.at[cls, slot, :, pl.ds(0, POSITIONS - 1)], x_recv_sem.at[cls, slot])
        for bit in (1, 0):
            row = flipped(group[cls][2], bit) * 2
            part[cls, offset * 2 + bit] = gram(
                xrecv[cls, slot, row], xrecv[cls, slot, row + 1]
            )

    def wait_single(cls, offset):
        slot = 3 - offset
        wait_bytes(xlast.at[cls, slot, :, pl.ds(0, POSITIONS - 1)], x_recv_sem.at[cls, 2 + slot])

    def arrived_gram(cls, offset):
        slot = 3 - offset
        part[cls, offset] = gram(xlast[cls, slot, 0], xlast[cls, slot, 1])

    def single_gram(cls, offset):
        wait_single(cls, offset)
        arrived_gram(cls, offset)

    def sem_of(cls, offset, piece):
        if offset == 0:
            return m_recv_sem.at[0]
        fed = [other for other in range(1, GROUPS) if feeders(other, piece)]
        return m_recv_sem.at[1 + (cls * 2 + piece) * 3 + fed.index(offset)]

    def wait_fed(cls, offset, piece):
        count = len(feeders(offset, piece))
        if count:
            wait_bytes(mrecv.at[cls, piece, pl.ds(0, count)], sem_of(cls, offset, piece))

    def wait_sums():
        wait_bytes(msend.at[pl.ds(0, 12)], sem_of(0, 0, 0))

    def gram_sum(cls, offset, piece):
        total = part[cls, offset, pl.ds(piece * PIECE, PIECE), :]
        for other in feeders(offset, piece):
            total = total + mrecv[cls, piece, other].astype(jnp.float32)
        return total

    def pass_on(cls, offset, piece):
        wait_fed(cls, offset, piece)
        at = cls * 16 + piece * GROUPS + offset
        msend[at] = gram_sum(cls, offset, piece).astype(jnp.bfloat16)
        pltpu.make_async_remote_copy(
            src_ref=msend.at[at],
            dst_ref=mrecv.at[cls, piece, offset],
            send_sem=m_send_sem,
            recv_sem=sem_of(cls, offset ^ next_bit(offset, piece), piece),
            device_id=place(1 - cls, next_bit(offset, piece)),
            device_id_type=MESH,
        ).start()

    for cls in range(2):
        pair_grams(cls, 3)
        pass_on(cls, 7, 1)
        pass_on(cls, 7, 0)
        pass_on(cls, 6, 0)
    send_single(2)
    for cls in range(2):
        pair_grams(cls, 2)
        pass_on(cls, 5, 1)
    send_single(1)
    wait_bytes(tpass.at[:, pl.ds(0, POSITIONS - 1)], t_sem.at[0, 1])
    along_groups(tpass, trecv, t_sem.at[1])
    for cls in range(2):
        pass_on(cls, 6, 1)
    for cls in range(2):
        pass_on(cls, 5, 0)
        pass_on(cls, 4, 0)
    for cls in range(2):
        single_gram(cls, 3)
        single_gram(cls, 2)
        pass_on(cls, 3, 1)
        pass_on(cls, 3, 0)
        pass_on(cls, 2, 0)
    send_single(0)
    for cls in range(2):
        pass_on(cls, 4, 1)
    for cls in range(2):
        single_gram(cls, 1)
        pass_on(cls, 1, 1)
        pass_on(cls, 1, 0)
    for cls in range(2):
        pass_on(cls, 2, 1)

    lane = lax.broadcasted_iota(jnp.int32, (16, 128), 1) // 32
    wait_bytes(trecv.at[pl.ds(0, GROUPS - 1)], t_sem.at[1, 1])
    for device in range(128):
        bits_v, bits_u, its_core = split_place(device // 8, device % 8)
        rows[device * 4 : device * 4 + 4, :] = trecv[
            number(bits_v), number(bits_u) * 2 + its_core
        ].astype(jnp.float32)
    for i in range(4):
        blocks = [rows[pl.ds(g * 4 + i, 16, stride=32), :] for g in range(8)]
        for t in range(4):
            for tile in range(2):
                total = jnp.zeros((16, 128), jnp.float32)
                for k in range(4):
                    turned = blocks[tile * 4 + k]
                    if k != t:
                        turned = pltpu.roll(turned, (32 * (k - t)) % 128, 1)
                    total = jnp.where(lane == k, turned, total)
                tmat[
                    i // 2, (i % 2) * 64 + t * 16 : (i % 2) * 64 + t * 16 + 16,
                    tile * 128 : tile * 128 + 128,
                ] = total.astype(jnp.bfloat16)

    for cls in range(2):
        wait_single(cls, 0)
    for cls in range(2):
        arrived_gram(cls, 0)

    bins = bins_of(v, u, core)

    def combine(straight, turned):
        return (
            0.5 * (straight[:64] - straight[64:] + turned[:64] + turned[64:]),
            0.5 * (straight[:64] + straight[64:] - turned[:64] + turned[64:]),
        )

    def halves(whole):
        high = whole.astype(jnp.bfloat16)
        return high, (whole - high.astype(jnp.float32)).astype(jnp.bfloat16)

    wait_sums()
    both_grams = [
        halves(jnp.concatenate([gram_sum(cls, 0, piece) for piece in range(2)], axis=0))
        for cls in range(2)
    ]
    both_once = []
    for cls in range(2):
        (high, low), left = both_grams[cls], tmat[cls]
        both_once.append(
            combine(nn(left, high) + nn(left, low), nt(left, high) + nt(left, low))
        )
    both_twice = []
    for cls in range(2):
        high, low = both_grams[cls]
        once_high, once_low = halves(jnp.concatenate(both_once[cls], axis=0))
        lines = jnp.concatenate([once_high, once_low], axis=0)
        straight, turned = nn(lines, high), nt(lines, high)
        both_twice.append(
            combine(
                straight[:128] + straight[128:] + nn(once_high, low),
                turned[:128] + turned[128:] + nt(once_high, low),
            )
        )
    for cls in range(2):
        load = loading[bins[cls]]
        step = 1.0 / (load + rho)
        keep, take = 2.0 * step - load * step * step, step * step
        for side in range(2):
            pred = keep * both_once[cls][side] - take * both_twice[cls][side]
            for g in range(8):
                k, tile = g % 4, g // 4
                moved = jnp.zeros((16, 128), jnp.float32)
                for t in range(4):
                    turned = pred[t * 16 : t * 16 + 16, tile * 128 : tile * 128 + 128]
                    if k != t:
                        turned = pltpu.roll(turned, (32 * (t - k)) % 128, 1)
                    moved = jnp.where(lane == t, turned, moved)
                rows[pl.ds(g * 4 + cls * 2 + side, 16, stride=32), :] = moved

    me = gx * 8 + gy
    for device in range(128):
        psend[device] = rows[device * 4 : device * 4 + 4, :].astype(jnp.bfloat16)
    for by_v, by_u, flip_core in FAR_FIRST:
        row, column = place_off(by_v, by_u, flip_core)
        pltpu.make_async_remote_copy(
            src_ref=psend.at[row * 8 + column],
            dst_ref=precv.at[me],
            send_sem=p_sem.at[0],
            recv_sem=p_sem.at[1],
            device_id=(row, column),
            device_id_type=MESH,
        ).start()
    precv[me] = psend[me]
    wait_bytes(precv.at[pl.ds(0, 127)], p_sem.at[1])
    for device in range(128):
        rows[device * 4 : device * 4 + 4, :] = precv[device].astype(jnp.float32)
    out[...] = rows[...].astype(jnp.bfloat16)

    wait_bytes(xsend.at[pl.ds(0, 32 * (POSITIONS - 1))], x_send_sem)
    wait_bytes(msend.at[pl.ds(0, 4 * (GROUPS - 1))], m_send_sem)
    wait_bytes(tpass.at[:, pl.ds(0, POSITIONS - 1)], t_sem.at[0, 0])
    wait_bytes(trecv.at[pl.ds(0, GROUPS - 1)], t_sem.at[1, 0])
    wait_bytes(precv.at[pl.ds(0, 127)], p_sem.at[0])


def tables(length):
    forward, inverse = transform_tables(length)
    by_pair = (
        forward.reshape(2, POSITIONS, 4, 4, length)
        .transpose(0, 2, 1, 3, 4)
        .reshape(8, POSITIONS * 4, length)
    )
    first = []
    bits = [(n // 4, n // 2 % 2, n % 2) for n in range(GROUPS)]
    for pos in range(POSITIONS):
        for grp in range(GROUPS):
            for found in bins_of(bits[grp], bits[pos // 2], pos % 2):
                first += [2 * found, 2 * found + 1]
    second = []
    for device in range(128):
        for found in bins_of(*split_place(device // 8, device % 8)):
            second += [2 * found, 2 * found + 1]
    return tuple(
        jnp.asarray(table).astype(jnp.bfloat16)
        for table in (by_pair, forward[first], inverse[second])
    )


def local(proof, target, loading):
    channels, segments, length = proof.shape
    rho = (1.0 + math.sqrt(2048 / segments)) ** 2
    by_pair, by_owner, inverse = tables(length)
    bf16, f32 = jnp.bfloat16, jnp.float32
    hbm = pl.BlockSpec(memory_space=pltpu.HBM)
    scratch = [
        pltpu.VMEM((8, 64, 512), bf16),
        pltpu.VMEM((512, 512), bf16),
        pltpu.VMEM((16, 256, 512), bf16),
        pltpu.VMEM((128, 512), bf16),
        pltpu.SMEM((256,), f32),
        pltpu.VMEM((2, CHANNELS * STRIDE, 128), f32),
        pltpu.VMEM((512, CHANNELS, 256), bf16),
        pltpu.VMEM((2, 2, 4, POSITIONS, CHANNELS, 256), bf16),
        pltpu.VMEM((2, 4, 2, POSITIONS, CHANNELS, 256), bf16),
        pltpu.VMEM((2, GROUPS, 256, 256), f32),
        pltpu.VMEM((4 * GROUPS, PIECE, 256), bf16),
        pltpu.VMEM((2, 2, GROUPS, PIECE, 256), bf16),
        pltpu.VMEM((2, 128, 256), bf16),
        pltpu.VMEM((POSITIONS, GROUPS, 4, 128), bf16),
        pltpu.VMEM((GROUPS, POSITIONS, 4, 128), bf16),
        pltpu.VMEM((GROUPS, POSITIONS, 4, 128), bf16),
        pltpu.VMEM((512, 128), f32),
        pltpu.VMEM((128, 4, 128), bf16),
        pltpu.VMEM((128, 4, 128), bf16),
        pltpu.SemaphoreType.DMA((3,)),
        pltpu.SemaphoreType.DMA((2,)),
        pltpu.SemaphoreType.DMA((3,)),
        pltpu.SemaphoreType.DMA,
        pltpu.SemaphoreType.DMA((2, 6)),
        pltpu.SemaphoreType.DMA,
        pltpu.SemaphoreType.DMA((13,)),
        pltpu.SemaphoreType.DMA((2, 2)),
        pltpu.SemaphoreType.DMA((2,)),
    ]
    hold = [
        pltpu.with_memory_space_constraint(array, pltpu.HBM)
        for array in (by_pair, by_owner, proof, target.reshape(128, length), loading)
    ]
    spectra = pl.pallas_call(
        functools.partial(kernel, rho),
        out_shape=jax.ShapeDtypeStruct((512, 128), bf16),
        in_specs=[hbm] * 5,
        out_specs=pl.BlockSpec(memory_space=pltpu.VMEM),
        scratch_shapes=scratch,
        compiler_params=pltpu.CompilerParams(
            collective_id=0, has_side_effects=True, vmem_limit_bytes=40 * 2**20
        ),
    )(*hold)
    return tn(spectra, inverse).reshape(4, 32, length)


def solution(mesh):
    return jax.shard_map(
        local,
        mesh=mesh,
        in_specs=(P(("gx", "gy"), None, None), P("gx", "gy", None), P()),
        out_specs=P("gx", "gy", None),
        check_vma=False,
    )
```
